32 devices in a mesh: irrep: 4 (over z), occ: 4 (over y, core), vir: 2 (over x).
Axes of the slice: x: 2, y: 2, z: 4, core: 2. Of those that a mesh axis runs over, the one named last changes fastest.
Arguments:
- amplitudes: bfloat16 [8, 320, 12288], P('irrep', None, ('occ', 'vir')), may hold values from -6 to 6
- ladder_ints: bfloat16 [8, 12288, 12288], P('irrep', ('occ', 'vir')), may hold values from -0.078125 to 0.078125
- hole_ints: bfloat16 [8, 320, 320], P('irrep'), may hold values from -0.3125 to 0.3125
- occ_energy: float32 [8, 320], P('irrep'), may hold values from -3 to -0.5
- vir_energy: float32 [8, 12288], P('irrep', ('occ', 'vir')), may hold values from 0.5 to 3
- occ_pairs: int32 [8], replicated, may hold values from 160 to 320, as said below
- vir_pairs: int32 [8], replicated, may hold values from 6144 to 12288, as said below
Outputs:
- updated: bfloat16 [8, 320, 12288], P('irrep', None, ('occ', 'vir'))
- residual_norm: float32 [8], P('irrep')
The draws below stay inside these ranges and needn't reach their ends.
Inputs may be any that keep to these rules, and one draw needn't show every extreme that they name: `occ_pairs`: some block has exactly 320 live occupied pairs in every draw. `vir_pairs`: some block has exactly 12288 live virtual pairs in every draw.
All inputs are finite; a program needn't handle non-finite values.
Results may differ from the reference program's by a relative error of at most 0.001.
Values may be sent and summed in bfloat16 or wider, within the bound.
A program may use at most 192 MiB of HBM per device.

```python
import jax
import jax.numpy as jnp

NB = 8
OP = 320
VP = 12288


def draw_occ_pairs(key, part):
    first_key, second_key = jax.random.split(jax.random.fold_in(key, 11))
    values = jax.random.randint(first_key, (NB,), OP // 2, OP + 1)
    chosen = jax.random.randint(second_key, (), 0, NB)
    return jnp.where(jnp.arange(NB) == chosen, OP, values).astype(jnp.int32)


def draw_vir_pairs(key, part):
    first_key, second_key = jax.random.split(jax.random.fold_in(key, 23))
    values = jax.random.randint(first_key, (NB,), VP // 2, VP + 1)
    chosen = jax.random.randint(second_key, (), 0, NB)
    return jnp.where(jnp.arange(NB) == chosen, VP, values).astype(jnp.int32)


def with_spikes(drawn, stream_key, source, target, shards_of, factor):
    def block_of(dim):
        return (jnp.arange(drawn.shape[dim]) // (drawn.shape[dim] // shards_of)).reshape((-1,) + (1,) * (drawn.ndim - 1 - dim))

    near = jax.random.permutation(stream_key, shards_of)[block_of(target)]
    second = (block_of(target) + shards_of // 2) % shards_of
    return jnp.where((block_of(source) == near) | (block_of(source) == second), factor * drawn, drawn)


def shard_levels(stream_key, shape, pieces, low, largest):
    def one(position, blocks):
        steps = jax.random.uniform(jax.random.fold_in(jax.random.fold_in(stream_key, 6), position), (blocks,), jnp.float32, low / len(pieces), largest / len(pieces))
        return jnp.repeat(jnp.exp(steps), shape[position] // blocks).reshape((-1,) + (1,) * (len(shape) - position - 1))

    gain = one(*pieces[0])
    for cut in pieces[1:]:
        gain = gain * one(*cut)
    return gain


def centred(stream_key, dims, scale, bound, cuts=(), kind=jnp.bfloat16):
    gain = shard_levels(stream_key, dims, cuts, -0.22, 0.18) if cuts else 1.0
    result = jax.random.normal(stream_key, dims, jnp.float32) * scale * gain
    return jnp.minimum(jnp.maximum(result, -bound), bound).astype(kind)


def heavy_noise(own_key, shape, deviation, bound, shards, heavy, kind=jnp.bfloat16):
    entries = deviation * jax.random.normal(own_key, shape, jnp.float32)
    if shards:
        entries = entries * shard_levels(own_key, shape, shards, -0.22, 0.18)
    return jnp.clip(with_spikes(entries, jax.random.fold_in(own_key, 3), *heavy), -bound, bound).astype(kind)


def setup_inputs(seed: int = 0) -> dict:
    splits = jax.random.split(jax.random.key(seed), 8)
    amplitudes = centred(splits[0], (NB, OP, VP), 1.0, 6.0, ((0, 4), (2, 8)))
    ladder_ints = heavy_noise(splits[1], (NB, VP, VP), VP ** -0.5, 0.078125, ((0, 4), (1, 8)), (1, 2, 8, 2.0))
    hole_ints = centred(splits[2], (NB, OP, OP), OP ** -0.5, 0.3125, ((0, 4),))
    occ_energy = jnp.clip(-3.0 + 2.5 * jax.random.uniform(splits[3], (NB, OP), jnp.float32) ** shard_levels(splits[3], (NB, OP), ((0, 4),), -0.2, 0.2), -3.0, -0.5)
    vir_energy = jnp.clip(0.5 + 2.5 * jax.random.uniform(splits[4], (NB, VP), jnp.float32) ** shard_levels(splits[4], (NB, VP), ((0, 4), (1, 8)), -0.2, 0.2), 0.5, 3.0)
    occ_pairs = draw_occ_pairs(jax.random.fold_in(splits[7], 71), 0)
    vir_pairs = draw_vir_pairs(jax.random.fold_in(splits[7], 71), 0)
    return dict(amplitudes=amplitudes, ladder_ints=ladder_ints, hole_ints=hole_ints, occ_energy=occ_energy, vir_energy=vir_energy, occ_pairs=occ_pairs, vir_pairs=vir_pairs)


LEVEL_SHIFT = 0.5
EPSILON = 1e-06

def reference(amplitudes, ladder_ints, hole_ints, occ_energy, vir_energy, occ_pairs, vir_pairs):
    row_index = jnp.arange(OP, dtype=jnp.int32)
    col_index = jnp.arange(VP, dtype=jnp.int32)
    results = []
    norms = []
    for block in range(NB):
        keep_mask = (row_index[:, None] < occ_pairs[block]) & (col_index[None, :] < vir_pairs[block])
        masked = jnp.where(keep_mask, amplitudes[block], jnp.zeros((), amplitudes.dtype))
        ladder_term = jnp.dot(masked, ladder_ints[block], preferred_element_type=jnp.float32)
        hole_term = jnp.dot(hole_ints[block], masked, preferred_element_type=jnp.float32)
        wide = masked.astype(jnp.float32)
        denominator = vir_energy[block][None, :] - occ_energy[block][:, None]
        residual = jnp.where(keep_mask, ladder_term + hole_term + denominator * wide, jnp.zeros((), jnp.float32))
        updated = wide - residual / (denominator + LEVEL_SHIFT)
        pair_count = (occ_pairs[block] * vir_pairs[block]).astype(jnp.float32)
        results.append(updated.astype(jnp.bfloat16))
        norms.append(jnp.sqrt(jnp.sum(residual * residual) / pair_count + EPSILON))
    return (jnp.stack(results), jnp.stack(norms))
```

```python
import functools

import jax
import jax.numpy as jnp
from jax import lax
from jax.experimental import pallas as pl
from jax.experimental.pallas import tpu as pltpu
from jax.sharding import PartitionSpec as P

LEVEL_SHIFT = 0.5
EPSILON = 1e-06
GRID_STEPS = 256.0
TOP = 32767.0
CODE_ROWS = 16
SLOTS = ("occ", "vir")
LANES = 128
VMEM_BYTES = 67043328
MESH = pl.DeviceIdType.MESH


def encode(value, out_ref):
    rows, cols = value.shape
    largest = jnp.max(jnp.abs(value), axis=0, keepdims=True)
    code = jnp.ceil(jnp.log2(jnp.maximum(largest, 1e-30)) * GRID_STEPS) + 1.0
    scaled = value * (jnp.exp2(code * (-1.0 / GRID_STEPS)) * TOP)
    out_ref[0:rows, :] = jnp.round(scaled).astype(jnp.int32).astype(jnp.int16)
    out_ref[rows : rows + CODE_ROWS, :] = (
        jnp.broadcast_to(code, (CODE_ROWS, cols)).astype(jnp.int32).astype(jnp.int16)
    )


def decode(in_ref):
    rows = in_ref.shape[0] - CODE_ROWS
    codes = in_ref[rows : rows + CODE_ROWS, :].astype(jnp.int32).astype(jnp.float32)
    scale = jnp.exp2(codes[0:1, :] * (1.0 / GRID_STEPS)) * (1.0 / TOP)
    return in_ref[0:rows, :].astype(jnp.int32).astype(jnp.float32) * scale


def ladder_kernel(received, coded, slot_ref, amp_ref, ladder_ref, *refs):
    out_ref = refs[-1]
    value = jnp.dot(amp_ref[0], ladder_ref[0], preferred_element_type=jnp.float32)
    for ref in refs[:received]:
        value = value + decode(ref)
    if coded:
        encode(value, out_ref)
    else:
        out_ref[...] = value


def tile_of(cols):
    return next(size for size in (768, 512, 384, 256, 128) if cols % size == 0)


def ladder_call(block, slot, masked, ladder, received, coded):
    _, rows, cols = masked.shape
    tile = tile_of(cols)
    steps = cols // tile
    out_rows, out_type = (rows + CODE_ROWS, jnp.int16) if coded else (rows, jnp.float32)
    return pl.pallas_call(
        functools.partial(ladder_kernel, len(received), coded),
        grid_spec=pltpu.PrefetchScalarGridSpec(
            num_scalar_prefetch=1,
            grid=(steps,),
            in_specs=[
                pl.BlockSpec((1, rows, cols), lambda j, slot: (block, 0, 0)),
                pl.BlockSpec((1, cols, tile), lambda j, slot: (block, 0, slot[0] * steps + j)),
            ]
            + [pl.BlockSpec((rows + CODE_ROWS, tile), lambda j, slot: (0, j))] * len(received),
            out_specs=pl.BlockSpec((out_rows, tile), lambda j, slot: (0, j)),
        ),
        out_shape=jax.ShapeDtypeStruct((out_rows, cols), out_type),
        cost_estimate=pl.CostEstimate(
            flops=2 * rows * cols * cols,
            bytes_accessed=2 * cols * cols + 4 * rows * cols * (1 + len(received)),
            transcendentals=0,
        ),
        name="ladder",
    )(slot.reshape(1), masked, ladder, *received)


def join_kernel(total_ref, *refs):
    value = total_ref[...]
    for ref in refs[:-1]:
        value = value + decode(ref)
    encode(value, refs[-1])


def join_call(total, received):
    rows, cols = total.shape
    tile = tile_of(cols)
    coded = pl.BlockSpec((rows + CODE_ROWS, tile), lambda j: (0, j))
    return pl.pallas_call(
        join_kernel,
        grid=(cols // tile,),
        in_specs=[pl.BlockSpec((rows, tile), lambda j: (0, j))] + [coded] * len(received),
        out_specs=coded,
        out_shape=jax.ShapeDtypeStruct((rows + CODE_ROWS, cols), jnp.int16),
        cost_estimate=pl.CostEstimate(
            flops=8 * rows * cols, bytes_accessed=(6 + 2 * len(received)) * rows * cols, transcendentals=0
        ),
        name="join",
    )(total, *received)


def final_kernel(blocks, parts, start_ref, occ_ref, vir_ref, amp_ref, hole_ref, occ_energy_ref, vir_energy_ref, *refs):
    out_ref, square_ref = refs[-2], refs[-1]
    rows, tile = out_ref.shape[1:]
    step = pl.program_id(0)
    column = start_ref[0] + step * tile + lax.broadcasted_iota(jnp.int32, (rows, tile), 1)
    row = lax.broadcasted_iota(jnp.int32, (rows, tile), 0)
    for block in range(blocks):
        mine = refs[block * parts : (block + 1) * parts]
        value = mine[0][...]
        for ref in mine[1:]:
            value = value + decode(ref)
        amp = amp_ref[block]
        value = value + jnp.dot(hole_ref[block], amp, preferred_element_type=jnp.float32)
        wide = amp.astype(jnp.float32)
        denominator = vir_energy_ref[block] - occ_energy_ref[block]
        keep = (row < occ_ref[block]) & (column < vir_ref[block])
        residual = jnp.where(keep, value + denominator * wide, 0.0)
        out_ref[block] = (wide - residual / (denominator + LEVEL_SHIFT)).astype(jnp.bfloat16)
        squares = jnp.sum((residual * residual).reshape(rows // 8, 8, tile), axis=0)
        squares = jnp.broadcast_to(jnp.sum(squares), (8, 128))

        @pl.when(step == 0)
        def _():
            square_ref[block] = squares

        @pl.when(step != 0)
        def _():
            square_ref[block] += squares


def final_call(start, occ_here, vir_here, masked, hole, occ_energy, vir_energy, operands):
    blocks, rows, cols = masked.shape
    parts = len(operands[0])
    tile = 512 if cols % 512 == 0 else tile_of(cols)
    total = pl.BlockSpec((rows, tile), lambda j, *_: (0, j))
    coded = pl.BlockSpec((rows + CODE_ROWS, tile), lambda j, *_: (0, j))
    return pl.pallas_call(
        functools.partial(final_kernel, blocks, parts),
        grid_spec=pltpu.PrefetchScalarGridSpec(
            num_scalar_prefetch=3,
            grid=(cols // tile,),
            in_specs=[
                pl.BlockSpec((blocks, rows, tile), lambda j, *_: (0, 0, j)),
                pl.BlockSpec((blocks, rows, rows), lambda j, *_: (0, 0, 0)),
                pl.BlockSpec((blocks, rows, 1), lambda j, *_: (0, 0, 0)),
                pl.BlockSpec((blocks, 1, tile), lambda j, *_: (0, 0, j)),
            ]
            + ([total] + [coded] * (parts - 1)) * blocks,
            out_specs=[
                pl.BlockSpec((blocks, rows, tile), lambda j, *_: (0, 0, j)),
                pl.BlockSpec((blocks, 8, 128), lambda j, *_: (0, 0, 0)),
            ],
        ),
        out_shape=[
            jax.ShapeDtypeStruct((blocks, rows, cols), jnp.bfloat16),
            jax.ShapeDtypeStruct((blocks, 8, 128), jnp.float32),
        ],
        cost_estimate=pl.CostEstimate(
            flops=2 * blocks * rows * rows * cols, bytes_accessed=12 * blocks * rows * cols, transcendentals=0
        ),
        name="final",
    )(
        start.reshape(1), occ_here, vir_here, masked, hole,
        occ_energy[:, :, None], vir_energy[:, None, :], *[x for group in operands for x in group],
    )


def table_lookup(table, block_ids):
    entries = table.shape[0]
    match = jnp.arange(entries, dtype=jnp.int32)[None, :] == block_ids[:, None]
    return jnp.sum(jnp.where(match, table[None, :], 0), axis=1)


def body(amplitudes, ladder_ints, hole_ints, occ_energy, vir_energy, occ_pairs, vir_pairs):
    blocks, rows, cols = amplitudes.shape
    occ_size, vir_size = lax.axis_size("occ"), lax.axis_size("vir")
    slots = occ_size * vir_size
    block_ids = lax.axis_index("irrep") * blocks + jnp.arange(blocks, dtype=jnp.int32)
    slot = lax.axis_index("occ") * vir_size + lax.axis_index("vir")
    start = slot * cols
    occ_here = table_lookup(occ_pairs, block_ids)
    vir_here = table_lookup(vir_pairs, block_ids)
    row = jnp.arange(rows, dtype=jnp.int32)
    column = start + jnp.arange(cols, dtype=jnp.int32)
    keep = (row[None, :, None] < occ_here[:, None, None]) & (column[None, None, :] < vir_here[:, None, None])
    masked = jnp.where(keep, amplitudes, jnp.zeros((), amplitudes.dtype))

    core = vir_size if occ_size > vir_size else 1
    bits = [1 << i for i in range(slots.bit_length() - 1) if 1 << i != core]

    def exchange(array, bit):
        return lax.ppermute(array, SLOTS, [(s, s ^ bit) for s in range(slots)])

    orders = [bits if block % 2 == 0 else bits[::-1] for block in range(blocks)]
    arrived = [{} for _ in range(blocks)]
    for rank in range((1 << len(bits)) - 1, -1, -1):
        chosen = [i for i in range(len(bits)) if rank >> (len(bits) - 1 - i) & 1]
        flips = [sum(order[i] for i in chosen) for order in orders]
        firsts = [ladder_call(b, slot ^ (flips[b] | core), masked, ladder_ints, [], True) for b in range(blocks)]
        firsts = [exchange(first, core) for first in firsts]
        for b in range(blocks):
            order, got = orders[b], arrived[b].get(flips[b], [])
            direct = bool(chosen) and not got
            total = ladder_call(b, slot ^ flips[b], masked, ladder_ints, [firsts[b]], direct)
            if not chosen:
                arrived[b][0] = [total] + got
                continue
            packed = total if direct else join_call(total, got)
            bit = order[chosen[0]]
            arrived[b].setdefault(flips[b] ^ bit, []).append(exchange(packed, bit))
    updated, squares = final_call(
        start, occ_here, vir_here, masked, hole_ints, occ_energy, vir_energy, [arrived[b][0] for b in range(blocks)]
    )
    summed_squares = lax.psum(squares[:, 0, 0], SLOTS)
    pair_count = (occ_here * vir_here).astype(jnp.float32)
    return updated, jnp.sqrt(summed_squares / pair_count + EPSILON)


def core_axis_is_low_bit_of_occ(occ_size, vir_size):
    return occ_size == 4 and vir_size == 2


def chunk_count(cols):
    return next(count for count in (3, 2, 1) if cols % (count * LANES) == 0)


def group_kernel(
    dims, occ_ref, vir_ref, amp_hbm, ladder_hbm, hole_hbm, occ_energy_ref, vir_energy_ref, out_hbm, norm_ref,
    amp, hole, occ_wide, lad, core_out, core_in, mine, base, link_out, link_in, result, squares, squares_in,
    amp_sem, hole_sem, lad_sem, core_send, core_recv, link_send, link_recv, out_sem, square_send, square_recv,
):
    rows, cols, chunks = dims
    tile = cols // chunks
    groups = tile // LANES
    steps = 4 * chunks
    x, o = lax.axis_index("vir"), lax.axis_index("occ")
    y, core = o // 2, o % 2
    me = o * 2 + x
    first = lax.axis_index("irrep") * 2
    across_core = {"occ": o + 1 - 2 * core}
    across_x = {"vir": 1 - x}
    across_y = {"occ": (o + 2) % 4}
    live_rows = [occ_ref[first + b] for b in range(2)]
    live_cols = [vir_ref[first + b] for b in range(2)]

    def remote(src, dst, send, recv, target):
        return pltpu.make_async_remote_copy(
            src_ref=src, dst_ref=dst, send_sem=send, recv_sem=recv, device_id=target, device_id_type=MESH
        )

    def lad_copy(step, b, role):
        phase, chunk = step // chunks, step % chunks
        flips = (1 - phase // 2, 1 - phase % 2)
        flip_x, flip_y = flips if b == 0 else flips[::-1]
        target_core = 1 - core if role == 0 else core
        target = (((y + flip_y) % 2) * 2 + target_core) * 2 + (x + flip_x) % 2
        slot = (step % 2) * 4 + role * 2 + b
        source = ladder_hbm.at[b, :, pl.ds(pl.multiple_of(target * cols + chunk * tile, LANES), tile)]
        return pltpu.make_async_copy(source, lad.at[slot], lad_sem.at[slot])

    def core_copy(step, b):
        slot = (step % 2) * 2 + b
        return remote(core_out.at[slot], core_in.at[step * 2 + b], core_send.at[slot], core_recv.at[step * 2 + b], across_core)

    def link_copy(step, b, target):
        at = step * 2 + b
        return remote(link_out.at[at], link_in.at[at], link_send.at[at], link_recv.at[at], target)

    def square_copy(index, sender, target):
        return remote(squares, squares_in.at[sender], square_send.at[index - 1], square_recv.at[sender], target)

    def square_source(index):
        return ((o + 4 - index // 2) % 4) * 2 + (x + index) % 2

    def peer(index):
        return {"occ": (o + index // 2) % 4, "vir": (x + index) % 2}

    amp_copies = [pltpu.make_async_copy(amp_hbm.at[b], amp.at[b], amp_sem.at[b]) for b in range(2)]
    hole_copy = pltpu.make_async_copy(hole_hbm, hole, hole_sem)
    amp_copies[0].start()
    for role in range(2):
        for b in range(2):
            lad_copy(0, b, role).start()
            if role == 0 and b == 0:
                amp_copies[1].start()
    for role in range(2):
        for b in range(2):
            lad_copy(1, b, role).start()
    hole_copy.start()

    barrier = pltpu.get_barrier_semaphore()
    for index in range(1, 8):
        pl.semaphore_signal(barrier, inc=1, device_id=peer(index), device_id_type=MESH)

    def keep_of(b, row0, height, column0, width):
        row = row0 + lax.broadcasted_iota(jnp.int32, (height, width), 0)
        column = me * cols + column0 + lax.broadcasted_iota(jnp.int32, (height, width), 1)
        return (row < live_rows[b]) & (column < live_cols[b])

    band = 32 if rows % 32 == 0 else 16

    def mask(b):
        amp_copies[b].wait()

        def one(index, carry):
            row0 = pl.multiple_of(index * band, band)
            part = amp[b, pl.ds(row0, band), :].astype(jnp.float32)
            part = jnp.where(keep_of(b, row0, band, 0, cols), part, 0.0)
            amp[b, pl.ds(row0, band), :] = part.astype(jnp.bfloat16)
            return carry

        lax.fori_loop(0, rows // band, one, 0)

    mask(0)
    mask(1)
    pl.semaphore_wait(barrier, 7)

    def part(b, slot):
        return jnp.dot(amp[b], lad[slot], preferred_element_type=jnp.float32)

    def produce(step):
        for b in range(2):
            slot = (step % 2) * 4 + b
            lad_copy(step, b, 0).wait()

            @pl.when(step >= 2)
            def _():
                core_copy(step - 2, b).wait_send()

            core_out[(step % 2) * 2 + b] = part(b, slot)
            core_copy(step, b).start()
        for b in range(2):
            slot = (step % 2) * 4 + 2 + b
            lad_copy(step, b, 1).wait()
            mine[b] = part(b, slot)

        @pl.when(step + 2 < steps)
        def _():
            for role in range(2):
                for b in range(2):
                    lad_copy(step + 2, b, role).start()

    def both_cores(step, b, g):
        lanes = slice(g * LANES, (g + 1) * LANES)
        return mine[b, :, lanes] + core_in[step * 2 + b, :, lanes]

    def scale_rows(at):
        codes = link_in[at, groups * rows : groups * rows + CODE_ROWS, :].astype(jnp.int32).astype(jnp.float32)
        return jnp.exp2(codes * (1.0 / GRID_STEPS)) * (1.0 / TOP)

    def decoded(at, scales, g):
        return link_in[at, g * rows : (g + 1) * rows, :].astype(jnp.int32).astype(jnp.float32) * scales[g : g + 1, :]

    def put(at, g, value, codes):
        largest = jnp.max(jnp.abs(value), axis=0, keepdims=True)
        code = jnp.ceil(jnp.log2(jnp.maximum(largest, 1e-30)) * GRID_STEPS) + 1.0
        scaled = value * (jnp.exp2(code * (-1.0 / GRID_STEPS)) * TOP)
        link_out[at, g * rows : (g + 1) * rows, :] = jnp.round(scaled).astype(jnp.int32).astype(jnp.int16)
        which = lax.broadcasted_iota(jnp.int32, (CODE_ROWS, LANES), 0)
        return jnp.where(which == g, jnp.broadcast_to(code, (CODE_ROWS, LANES)), codes)

    def put_codes(at, codes):
        link_out[at, groups * rows : groups * rows + CODE_ROWS, :] = codes.astype(jnp.int32).astype(jnp.int16)

    def send_own(step, carry):
        produce(step)
        for b in range(2):
            core_copy(step, b).wait_recv()
            at = step * 2 + b
            codes = jnp.zeros((CODE_ROWS, LANES), jnp.float32)
            for g in range(groups):
                codes = put(at, g, both_cores(step, b, g), codes)
            put_codes(at, codes)
            link_copy(step, b, across_x if b == 0 else across_y).start()
        return carry

    def send_joined(step, carry):
        produce(step)
        for b in range(2):
            core_copy(step, b).wait_recv()
            earlier = step - 2 * chunks
            link_copy(earlier, b, across_x if b == 0 else across_y).wait_recv()
            at = step * 2 + b
            scales = scale_rows(earlier * 2 + b)
            codes = jnp.zeros((CODE_ROWS, LANES), jnp.float32)
            for g in range(groups):
                codes = put(at, g, both_cores(step, b, g) + decoded(earlier * 2 + b, scales, g), codes)
            put_codes(at, codes)
            link_copy(step, b, across_y if b == 0 else across_x).start()
        return carry

    def gap_of(b, column):
        return vir_energy_ref[pl.ds(b, 1), pl.ds(column, LANES)] - occ_wide[b]

    def keep_base(step, carry):
        produce(step)
        chunk = step - 3 * chunks
        for b in range(2):
            column = pl.multiple_of(chunk * tile, LANES)
            from_hole = jnp.dot(hole[b], amp[b, :, pl.ds(column, tile)], preferred_element_type=jnp.float32)
            core_copy(step, b).wait_recv()
            for g in range(groups):
                lanes = slice(g * LANES, (g + 1) * LANES)
                at = pl.multiple_of(column + g * LANES, LANES)
                wide = amp[b, :, pl.ds(at, LANES)].astype(jnp.float32)
                base[chunk * 2 + b, :, lanes] = both_cores(step, b, g) + from_hole[:, lanes] + gap_of(b, at) * wide
        return carry

    lax.fori_loop(0, 2 * chunks, send_own, 0)
    lax.fori_loop(2 * chunks, 3 * chunks, send_joined, 0)

    hole_copy.wait()
    for b in range(2):
        occ_wide[b] = jnp.broadcast_to(occ_energy_ref[b : b + 1, :], (LANES, rows)).T
    lax.fori_loop(3 * chunks, 4 * chunks, keep_base, 0)

    def finish(chunk, carry):
        sums = list(carry)
        for b in range(2):
            near, far = chunks + chunk, 2 * chunks + chunk
            link_copy(near, b, across_x if b == 0 else across_y).wait_recv()
            link_copy(far, b, across_y if b == 0 else across_x).wait_recv()
            near_scales, far_scales = scale_rows(near * 2 + b), scale_rows(far * 2 + b)
            for g in range(groups):
                lanes = slice(g * LANES, (g + 1) * LANES)
                at = pl.multiple_of(chunk * tile + g * LANES, LANES)
                total = base[chunk * 2 + b, :, lanes] + decoded(near * 2 + b, near_scales, g)
                total = total + decoded(far * 2 + b, far_scales, g)
                residual = jnp.where(keep_of(b, 0, rows, at, LANES), total, 0.0)
                wide = amp[b, :, pl.ds(at, LANES)].astype(jnp.float32)
                result[chunk * 2 + b, :, lanes] = (wide - residual / (gap_of(b, at) + LEVEL_SHIFT)).astype(jnp.bfloat16)
                sums[b] = sums[b] + jnp.sum((residual * residual).reshape(rows // 8, 8, LANES), axis=0)
            out_copy(chunk, b).start()
        return tuple(sums)

    def out_copy(chunk, b):
        target = out_hbm.at[b, :, pl.ds(pl.multiple_of(chunk * tile, LANES), tile)]
        return pltpu.make_async_copy(result.at[chunk * 2 + b], target, out_sem.at[chunk * 2 + b])

    empty = jnp.zeros((8, LANES), jnp.float32)
    sums = lax.fori_loop(0, chunks, finish, (empty, empty))
    for b in range(2):
        squares[b] = sums[b]
        squares_in[me, b] = sums[b]
    for index in range(1, 8):
        square_copy(index, me, peer(index)).start()
    for index in range(1, 8):
        square_copy(index, square_source(index), peer(index)).wait_recv()
    for b in range(2):
        total = squares_in[0, b]
        for index in range(1, 8):
            total = total + squares_in[index, b]
        total = jnp.sum(total)
        count = (live_rows[b] * live_cols[b]).astype(jnp.float32)
        mean = jnp.full((8, LANES), total, jnp.float32) / jnp.full((8, LANES), count, jnp.float32)
        norm_ref[b] = jnp.sqrt(mean + EPSILON)[0, 0]

    def close(step, carry):
        for b in range(2):
            link_copy(step, b, across_x).wait_send()
        return carry

    lax.fori_loop(0, 3 * chunks, close, 0)
    for step in (steps - 2, steps - 1):
        for b in range(2):
            core_copy(step, b).wait_send()
    for index in range(1, 8):
        square_copy(index, me, peer(index)).wait_send()
    for chunk in range(chunks):
        for b in range(2):
            out_copy(chunk, b).wait()


def group_body(amplitudes, ladder_ints, hole_ints, occ_energy, vir_energy, occ_pairs, vir_pairs):
    blocks, rows, cols = amplitudes.shape
    chunks = chunk_count(cols)
    tile = cols // chunks
    coded_rows = (tile // LANES) * rows + CODE_ROWS
    anywhere = pl.BlockSpec(memory_space=pl.ANY)
    vmem = pl.BlockSpec(memory_space=pltpu.VMEM)
    smem = pl.BlockSpec(memory_space=pltpu.SMEM)
    dma = pltpu.SemaphoreType.DMA
    return pl.pallas_call(
        functools.partial(group_kernel, (rows, cols, chunks)),
        in_specs=[smem, smem, anywhere, anywhere, anywhere, vmem, vmem],
        out_specs=[anywhere, smem],
        out_shape=[
            jax.ShapeDtypeStruct((blocks, rows, cols), jnp.bfloat16),
            jax.ShapeDtypeStruct((blocks,), jnp.float32),
        ],
        scratch_shapes=[
            pltpu.VMEM((2, rows, cols), jnp.bfloat16),
            pltpu.VMEM((2, rows, rows), jnp.bfloat16),
            pltpu.VMEM((2, rows, LANES), jnp.float32),
            pltpu.VMEM((8, cols, tile), jnp.bfloat16),
            pltpu.VMEM((4, rows, tile), jnp.float32),
            pltpu.VMEM((8 * chunks, rows, tile), jnp.float32),
            pltpu.VMEM((2, rows, tile), jnp.float32),
            pltpu.VMEM((2 * chunks, rows, tile), jnp.float32),
            pltpu.VMEM((6 * chunks, coded_rows, LANES), jnp.int16),
            pltpu.VMEM((6 * chunks, coded_rows, LANES), jnp.int16),
            pltpu.VMEM((2 * chunks, rows, tile), jnp.bfloat16),
            pltpu.VMEM((2, 8, LANES), jnp.float32),
            pltpu.VMEM((8, 2, 8, LANES), jnp.float32),
            dma((2,)), dma(()), dma((8,)), dma((4,)), dma((8 * chunks,)), dma((6 * chunks,)), dma((6 * chunks,)),
            dma((2 * chunks,)), dma((7,)), dma((8,)),
        ],
        compiler_params=pltpu.CompilerParams(
            collective_id=0, has_side_effects=True, vmem_limit_bytes=VMEM_BYTES
        ),
        name="ladder_group",
    )(occ_pairs, vir_pairs, amplitudes, ladder_ints, hole_ints, occ_energy, vir_energy)


def solution(mesh):
    in_specs = (
        P("irrep", None, SLOTS),
        P("irrep", SLOTS, None),
        P("irrep", None, None),
        P("irrep", None),
        P("irrep", SLOTS),
        P(),
        P(),
    )
    out_specs = (P("irrep", None, SLOTS), P("irrep"))
    small = core_axis_is_low_bit_of_occ(mesh.shape["occ"], mesh.shape["vir"])
    return jax.shard_map(group_body if small else body, mesh=mesh, in_specs=in_specs, out_specs=out_specs, check_vma=False)
```

```python
import functools

import jax
import jax.numpy as jnp
from jax import lax
from jax.experimental import pallas as pl
from jax.experimental.pallas import tpu as pltpu
from jax.sharding import PartitionSpec as P

LEVEL_SHIFT = 0.5
EPSILON = 1e-06
GRID_STEPS = 256.0
TOP = 32767.0
CODE_ROWS = 16
SLOTS = ("occ", "vir")
LANES = 128
VMEM_BYTES = 58 * 2**20
MESH = pl.DeviceIdType.MESH


def encode(value, out_ref):
    rows, cols = value.shape
    largest = jnp.max(jnp.abs(value), axis=0, keepdims=True)
    code = jnp.ceil(jnp.log2(jnp.maximum(largest, 1e-30)) * GRID_STEPS) + 1.0
    scaled = value * (jnp.exp2(code * (-1.0 / GRID_STEPS)) * TOP)
    out_ref[0:rows, :] = jnp.round(scaled).astype(jnp.int32).astype(jnp.int16)
    out_ref[rows : rows + CODE_ROWS, :] = (
        jnp.broadcast_to(code, (CODE_ROWS, cols)).astype(jnp.int32).astype(jnp.int16)
    )


def decode(in_ref):
    rows = in_ref.shape[0] - CODE_ROWS
    codes = in_ref[rows : rows + CODE_ROWS, :].astype(jnp.int32).astype(jnp.float32)
    scale = jnp.exp2(codes[0:1, :] * (1.0 / GRID_STEPS)) * (1.0 / TOP)
    return in_ref[0:rows, :].astype(jnp.int32).astype(jnp.float32) * scale


def ladder_kernel(received, coded, slot_ref, amp_ref, ladder_ref, *refs):
    out_ref = refs[-1]
    value = jnp.dot(amp_ref[0], ladder_ref[0], preferred_element_type=jnp.float32)
    for ref in refs[:received]:
        value = value + decode(ref)
    if coded:
        encode(value, out_ref)
    else:
        out_ref[...] = value


def tile_of(cols):
    return next(size for size in (768, 512, 384, 256, 128) if cols % size == 0)


def ladder_call(block, slot, masked, ladder, received, coded):
    _, rows, cols = masked.shape
    tile = tile_of(cols)
    steps = cols // tile
    out_rows, out_type = (rows + CODE_ROWS, jnp.int16) if coded else (rows, jnp.float32)
    return pl.pallas_call(
        functools.partial(ladder_kernel, len(received), coded),
        grid_spec=pltpu.PrefetchScalarGridSpec(
            num_scalar_prefetch=1,
            grid=(steps,),
            in_specs=[
                pl.BlockSpec((1, rows, cols), lambda j, slot: (block, 0, 0)),
                pl.BlockSpec((1, cols, tile), lambda j, slot: (block, 0, slot[0] * steps + j)),
            ]
            + [pl.BlockSpec((rows + CODE_ROWS, tile), lambda j, slot: (0, j))] * len(received),
            out_specs=pl.BlockSpec((out_rows, tile), lambda j, slot: (0, j)),
        ),
        out_shape=jax.ShapeDtypeStruct((out_rows, cols), out_type),
        cost_estimate=pl.CostEstimate(
            flops=2 * rows * cols * cols,
            bytes_accessed=2 * cols * cols + 4 * rows * cols * (1 + len(received)),
            transcendentals=0,
        ),
        name="ladder",
    )(slot.reshape(1), masked, ladder, *received)


def join_kernel(total_ref, *refs):
    value = total_ref[...]
    for ref in refs[:-1]:
        value = value + decode(ref)
    encode(value, refs[-1])


def join_call(total, received):
    rows, cols = total.shape
    tile = tile_of(cols)
    coded = pl.BlockSpec((rows + CODE_ROWS, tile), lambda j: (0, j))
    return pl.pallas_call(
        join_kernel,
        grid=(cols // tile,),
        in_specs=[pl.BlockSpec((rows, tile), lambda j: (0, j))] + [coded] * len(received),
        out_specs=coded,
        out_shape=jax.ShapeDtypeStruct((rows + CODE_ROWS, cols), jnp.int16),
        cost_estimate=pl.CostEstimate(
            flops=8 * rows * cols, bytes_accessed=(6 + 2 * len(received)) * rows * cols, transcendentals=0
        ),
        name="join",
    )(total, *received)


def final_kernel(blocks, parts, start_ref, occ_ref, vir_ref, amp_ref, hole_ref, occ_energy_ref, vir_energy_ref, *refs):
    out_ref, square_ref = refs[-2], refs[-1]
    rows, tile = out_ref.shape[1:]
    step = pl.program_id(0)
    column = start_ref[0] + step * tile + lax.broadcasted_iota(jnp.int32, (rows, tile), 1)
    row = lax.broadcasted_iota(jnp.int32, (rows, tile), 0)
    for block in range(blocks):
        mine = refs[block * parts : (block + 1) * parts]
        value = mine[0][...]
        for ref in mine[1:]:
            value = value + decode(ref)
        amp = amp_ref[block]
        value = value + jnp.dot(hole_ref[block], amp, preferred_element_type=jnp.float32)
        wide = amp.astype(jnp.float32)
        denominator = vir_energy_ref[block] - occ_energy_ref[block]
        keep = (row < occ_ref[block]) & (column < vir_ref[block])
        residual = jnp.where(keep, value + denominator * wide, 0.0)
        out_ref[block] = (wide - residual / (denominator + LEVEL_SHIFT)).astype(jnp.bfloat16)
        squares = jnp.sum((residual * residual).reshape(rows // 8, 8, tile), axis=0)
        squares = jnp.broadcast_to(jnp.sum(squares), (8, 128))

        @pl.when(step == 0)
        def _():
            square_ref[block] = squares

        @pl.when(step != 0)
        def _():
            square_ref[block] += squares


def final_call(start, occ_here, vir_here, masked, hole, occ_energy, vir_energy, operands):
    blocks, rows, cols = masked.shape
    parts = len(operands[0])
    tile = 512 if cols % 512 == 0 else tile_of(cols)
    total = pl.BlockSpec((rows, tile), lambda j, *_: (0, j))
    coded = pl.BlockSpec((rows + CODE_ROWS, tile), lambda j, *_: (0, j))
    return pl.pallas_call(
        functools.partial(final_kernel, blocks, parts),
        grid_spec=pltpu.PrefetchScalarGridSpec(
            num_scalar_prefetch=3,
            grid=(cols // tile,),
            in_specs=[
                pl.BlockSpec((blocks, rows, tile), lambda j, *_: (0, 0, j)),
                pl.BlockSpec((blocks, rows, rows), lambda j, *_: (0, 0, 0)),
                pl.BlockSpec((blocks, rows, 1), lambda j, *_: (0, 0, 0)),
                pl.BlockSpec((blocks, 1, tile), lambda j, *_: (0, 0, j)),
            ]
            + ([total] + [coded] * (parts - 1)) * blocks,
            out_specs=[
                pl.BlockSpec((blocks, rows, tile), lambda j, *_: (0, 0, j)),
                pl.BlockSpec((blocks, 8, 128), lambda j, *_: (0, 0, 0)),
            ],
        ),
        out_shape=[
            jax.ShapeDtypeStruct((blocks, rows, cols), jnp.bfloat16),
            jax.ShapeDtypeStruct((blocks, 8, 128), jnp.float32),
        ],
        cost_estimate=pl.CostEstimate(
            flops=2 * blocks * rows * rows * cols, bytes_accessed=12 * blocks * rows * cols, transcendentals=0
        ),
        name="final",
    )(
        start.reshape(1), occ_here, vir_here, masked, hole,
        occ_energy[:, :, None], vir_energy[:, None, :], *[x for group in operands for x in group],
    )


def table_lookup(table, block_ids):
    entries = table.shape[0]
    match = jnp.arange(entries, dtype=jnp.int32)[None, :] == block_ids[:, None]
    return jnp.sum(jnp.where(match, table[None, :], 0), axis=1)


def body(amplitudes, ladder_ints, hole_ints, occ_energy, vir_energy, occ_pairs, vir_pairs):
    blocks, rows, cols = amplitudes.shape
    occ_size, vir_size = lax.axis_size("occ"), lax.axis_size("vir")
    slots = occ_size * vir_size
    block_ids = lax.axis_index("irrep") * blocks + jnp.arange(blocks, dtype=jnp.int32)
    slot = lax.axis_index("occ") * vir_size + lax.axis_index("vir")
    start = slot * cols
    occ_here = table_lookup(occ_pairs, block_ids)
    vir_here = table_lookup(vir_pairs, block_ids)
    row = jnp.arange(rows, dtype=jnp.int32)
    column = start + jnp.arange(cols, dtype=jnp.int32)
    keep = (row[None, :, None] < occ_here[:, None, None]) & (column[None, None, :] < vir_here[:, None, None])
    masked = jnp.where(keep, amplitudes, jnp.zeros((), amplitudes.dtype))

    core = vir_size if occ_size > vir_size else 1
    bits = [1 << i for i in range(slots.bit_length() - 1) if 1 << i != core]

    def exchange(array, bit):
        return lax.ppermute(array, SLOTS, [(s, s ^ bit) for s in range(slots)])

    orders = [bits if block % 2 == 0 else bits[::-1] for block in range(blocks)]
    arrived = [{} for _ in range(blocks)]
    for rank in range((1 << len(bits)) - 1, -1, -1):
        chosen = [i for i in range(len(bits)) if rank >> (len(bits) - 1 - i) & 1]
        flips = [sum(order[i] for i in chosen) for order in orders]
        firsts = [ladder_call(b, slot ^ (flips[b] | core), masked, ladder_ints, [], True) for b in range(blocks)]
        firsts = [exchange(first, core) for first in firsts]
        for b in range(blocks):
            order, got = orders[b], arrived[b].get(flips[b], [])
            direct = bool(chosen) and not got
            total = ladder_call(b, slot ^ flips[b], masked, ladder_ints, [firsts[b]], direct)
            if not chosen:
                arrived[b][0] = [total] + got
                continue
            packed = total if direct else join_call(total, got)
            bit = order[chosen[0]]
            arrived[b].setdefault(flips[b] ^ bit, []).append(exchange(packed, bit))
    updated, squares = final_call(
        start, occ_here, vir_here, masked, hole_ints, occ_energy, vir_energy, [arrived[b][0] for b in range(blocks)]
    )
    summed_squares = lax.psum(squares[:, 0, 0], SLOTS)
    pair_count = (occ_here * vir_here).astype(jnp.float32)
    return updated, jnp.sqrt(summed_squares / pair_count + EPSILON)


def fits_group(mesh, cols):
    return mesh.shape["occ"] == 4 and mesh.shape["vir"] == 2 and cols % (6 * LANES) == 0


def group_kernel(
    dims, occ_hbm, vir_hbm, amp_hbm, ladder_hbm, hole_hbm, occ_energy_hbm, vir_energy_hbm, out_ref, squares_in, counts_ref,
    amp, hole, occ_wide, lad, core_out_small, core_out, core_in_small, core_in, mine, squares,
    occ_ref, vir_ref, occ_energy_ref, vir_energy_ref, pair_sem, energy_sem,
    amp_sem, hole_sem, lad_sem, core_send_small, core_send, core_recv_small, core_recv, square_send, square_recv, *links,
):
    rows, cols = dims
    big = cols // 2
    small = big // 3
    first_big, steps, lad_slots = 3, 10, lad.shape[0]
    outs, ins, sends, recvs = links[0:4], links[4:8], links[8:12], links[12:16]
    SMALL, WHOLE, HEAD, LAST = range(4)
    widths = (small, big, big - small, small)
    x, o = lax.axis_index("vir"), lax.axis_index("occ")
    y, core = o // 2, o % 2
    me = o * 2 + x
    first = lax.axis_index("irrep") * 2
    across_core = {"occ": o + 1 - 2 * core}
    across_x = {"vir": 1 - x}
    across_y = {"occ": (o + 2) % 4}
    near_side, far_side = (across_x, across_y), (across_y, across_x)

    def remote(src, dst, send, recv, target):
        return pltpu.make_async_remote_copy(
            src_ref=src, dst_ref=dst, send_sem=send, recv_sem=recv, device_id=target, device_id_type=MESH
        )

    def lad_copy(step, k, is_small):
        b, role = k % 2, k // 2
        half = step - first_big + 1
        phase = 0 if is_small else half // 2
        column = step * small if is_small else (half % 2) * big
        flips = (1 - phase // 2, 1 - phase % 2)
        flip_x, flip_y = flips if b == 0 else flips[::-1]
        target_core = 1 - core if role == 0 else core
        target = (((y + flip_y) % 2) * 2 + target_core) * 2 + (x + flip_x) % 2
        slot = (4 * step + k) % lad_slots
        width = small if is_small else big
        source = ladder_hbm.at[b, :, pl.ds(pl.multiple_of(target * cols + column, LANES), width)]
        return pltpu.make_async_copy(source, lad.at[slot, :, pl.ds(0, width)], lad_sem.at[slot])

    def core_copy(step, b, is_small):
        if is_small:
            at = step * 2 + b
            return remote(core_out_small.at[at], core_in_small.at[at], core_send_small.at[at], core_recv_small.at[at], across_core)
        slot, at = (step % 2) * 2 + b, (step - first_big) * 2 + b
        return remote(core_out.at[slot], core_in.at[at], core_send.at[slot], core_recv.at[at], across_core)

    def link_copy(kind, at, target):
        return remote(outs[kind].at[at], ins[kind].at[at], sends[kind].at[at], recvs[kind].at[at], target)

    def square_copy(index, sender, target):
        return remote(squares, squares_in.at[sender], square_send.at[index - 1], square_recv.at[sender], target)

    def square_source(index):
        return ((o + 4 - index // 2) % 4) * 2 + (x + index) % 2

    def peer(index):
        return {"occ": (o + index // 2) % 4, "vir": (x + index) % 2}

    amp_copies = [pltpu.make_async_copy(amp_hbm.at[b], amp.at[b], amp_sem.at[b]) for b in range(2)]
    hole_copy = pltpu.make_async_copy(hole_hbm, hole, hole_sem)
    pair_copies = [
        pltpu.make_async_copy(occ_hbm, occ_ref, pair_sem.at[0]), pltpu.make_async_copy(vir_hbm, vir_ref, pair_sem.at[1])
    ]
    energy_copies = [
        pltpu.make_async_copy(occ_energy_hbm, occ_energy_ref, energy_sem.at[0]),
        pltpu.make_async_copy(vir_energy_hbm, vir_energy_ref, energy_sem.at[1]),
    ]
    barrier = pltpu.get_barrier_semaphore()
    for index in range(1, 8):
        pl.semaphore_signal(barrier, inc=1, device_id=peer(index), device_id_type=MESH)
    for copy in pair_copies:
        copy.start()
    for b in range(2):
        amp_copies[b].start()
        lad_copy(0, b, True).start()
    for copy in pair_copies:
        copy.wait()
    live_rows = [occ_ref[first + b] for b in range(2)]
    live_cols = [vir_ref[first + b] for b in range(2)]

    def keep_of(b, column0, width):
        row = lax.broadcasted_iota(jnp.int32, (rows, width), 0)
        column = me * cols + column0 + lax.broadcasted_iota(jnp.int32, (rows, width), 1)
        return (row < live_rows[b]) & (column < live_cols[b])

    def mask(b):
        amp_copies[b].wait()
        shape = (16, LANES)
        lane = me * cols + lax.broadcasted_iota(jnp.int32, shape, 1)
        masks = [
            jnp.where(lane + g * LANES < live_cols[b], 1.0, 0.0).astype(jnp.bfloat16) for g in range(cols // LANES)
        ]

        def one(index, carry):
            row0 = pl.multiple_of(index * 16, 16)
            row = row0 + lax.broadcasted_iota(jnp.int32, shape, 0)
            live = jnp.where(row < live_rows[b], 1.0, 0.0).astype(jnp.bfloat16)
            for g in range(cols // LANES):
                lanes = slice(g * LANES, (g + 1) * LANES)
                amp[b, pl.ds(row0, 16), lanes] = amp[b, pl.ds(row0, 16), lanes] * masks[g] * live
            return carry

        lax.fori_loop(0, rows // 16, one, 0)

    mask(0)
    for n in range(2, lad_slots):
        lad_copy(n // 4, n % 4, True).start()
    mask(1)
    hole_copy.start()
    for copy in energy_copies:
        copy.start()
    pl.semaphore_wait(barrier, 7)

    def part(step, k, is_small):
        lad_copy(step, k, is_small).wait()
        width = small if is_small else big
        return jnp.dot(amp[k % 2], lad[(4 * step + k) % lad_slots, :, 0:width], preferred_element_type=jnp.float32)

    def refill(step, k, is_small):
        ahead = 4 * step + k + lad_slots
        later, k_later = step + (k + lad_slots) // 4, (k + lad_slots) % 4
        if is_small:

            @pl.when(later < first_big)
            def _():
                lad_copy(later, k_later, True).start()

            @pl.when(later >= first_big)
            def _():
                lad_copy(later, k_later, False).start()
        else:

            @pl.when(later < steps)
            def _():
                lad_copy(later, k_later, False).start()

    def produce(step, is_small):
        for b in range(2):
            if is_small:
                core_out_small[step * 2 + b] = part(step, b, True)
            else:

                @pl.when(step >= first_big + 2)
                def _():
                    core_copy(step - 2, b, False).wait_send()

                core_out[(step % 2) * 2 + b] = part(step, b, False)
            core_copy(step, b, is_small).start()
            refill(step, b, is_small)
        for b in range(2):
            width = small if is_small else big
            mine[b, :, 0:width] = part(step, 2 + b, is_small)
            refill(step, 2 + b, is_small)

    def lanes_of(g):
        return slice(g * LANES, (g + 1) * LANES)

    def both_cores(step, b, g, is_small):
        source, at = (core_in_small, step * 2 + b) if is_small else (core_in, (step - first_big) * 2 + b)
        return mine[b, :, lanes_of(g)] + source[at, :, lanes_of(g)]

    def scales_of(kind, at):
        top = widths[kind] // LANES * rows
        codes = ins[kind][at, top : top + CODE_ROWS, :].astype(jnp.int32).astype(jnp.float32)
        return jnp.exp2(codes * (1.0 / GRID_STEPS)) * (1.0 / TOP)

    def decoded(kind, at, scales, g):
        return ins[kind][at, g * rows : (g + 1) * rows, :].astype(jnp.int32).astype(jnp.float32) * scales[g : g + 1, :]

    def send(kind, at, values, target):
        out = outs[kind]
        codes = jnp.zeros((CODE_ROWS, LANES), jnp.float32)
        which = lax.broadcasted_iota(jnp.int32, (CODE_ROWS, LANES), 0)
        groups = widths[kind] // LANES
        for g in range(groups):
            value = values(g)
            largest = jnp.max(jnp.abs(value), axis=0, keepdims=True)
            code = jnp.ceil(jnp.log2(jnp.maximum(largest, 1e-30)) * GRID_STEPS) + 1.0
            scaled = value * (jnp.exp2(code * (-1.0 / GRID_STEPS)) * TOP)
            out[at, g * rows : (g + 1) * rows, :] = jnp.round(scaled).astype(jnp.int32).astype(jnp.int16)
            codes = jnp.where(which == g, jnp.broadcast_to(code, (CODE_ROWS, LANES)), codes)
        out[at, groups * rows : groups * rows + CODE_ROWS, :] = codes.astype(jnp.int32).astype(jnp.int16)
        link_copy(kind, at, target).start()

    def send_small(step, carry):
        produce(step, True)
        for b in range(2):
            core_copy(step, b, True).wait_recv()
            send(SMALL, step * 2 + b, lambda g: both_cores(step, b, g, True), near_side[b])
        return carry

    def send_whole(step, carry):
        produce(step, False)
        for b in range(2):
            core_copy(step, b, False).wait_recv()
            at = (step - first_big) * 2 + b
            send(WHOLE, at, lambda g: both_cores(step, b, g, False), near_side[b])
        return carry

    def send_joined(half):
        step = first_big + 3 + half
        produce(step, False)
        for b in range(2):
            core_copy(step, b, False).wait_recv()
            if half == 0:
                pieces = [(SMALL, 2 * piece + b, small // LANES) for piece in range(3)]
            else:
                pieces = [(WHOLE, b, big // LANES)]
            arrived = []
            for kind, at, groups in pieces:
                link_copy(kind, at, near_side[b]).wait_recv()
                scales = scales_of(kind, at)
                arrived += [(kind, at, scales, g) for g in range(groups)]

            def value(g):
                return both_cores(step, b, g, False) + decoded(*arrived[g])

            head = widths[HEAD] // LANES
            send(HEAD, half * 2 + b, value, far_side[b])
            send(LAST, half * 2 + b, lambda g: value(head + g), far_side[b])

    def gap_of(b, column):
        return vir_energy_ref[pl.ds(b, 1), pl.ds(column, LANES)] - occ_wide[b]

    def keep_base(step, carry):
        produce(step, False)
        start = (step - (steps - 2)) * big
        for b in range(2):
            from_hole = jnp.dot(
                hole[b], amp[b, :, pl.ds(pl.multiple_of(start, LANES), big)], preferred_element_type=jnp.float32
            )
            core_copy(step, b, False).wait_recv()
            for g in range(big // LANES):
                at = pl.multiple_of(start + g * LANES, LANES)
                wide = amp[b, :, pl.ds(at, LANES)].astype(jnp.float32)
                total = both_cores(step, b, g, False) + from_hole[:, lanes_of(g)] + gap_of(b, at) * wide
                core_in[(step - first_big) * 2 + b, :, lanes_of(g)] = total
        return carry

    def settle(half, carry):
        for b in range(2):
            at = (1 + half) * 2 + b
            link_copy(WHOLE, at, near_side[b]).wait_recv()
            scales = scales_of(WHOLE, at)
            base = (steps - 2 - first_big + half) * 2 + b
            for g in range(big // LANES):
                core_in[base, :, lanes_of(g)] = core_in[base, :, lanes_of(g)] + decoded(WHOLE, at, scales, g)
        return carry

    def residual_of(kind, half, skip, sums):
        for b in range(2):
            link_copy(kind, half * 2 + b, far_side[b]).wait_recv()
            scales = scales_of(kind, half * 2 + b)
            base = (steps - 2 - first_big + half) * 2 + b
            for g in range(widths[kind] // LANES):
                at = pl.multiple_of(half * big + (skip + g) * LANES, LANES)
                total = core_in[base, :, lanes_of(skip + g)] + decoded(kind, half * 2 + b, scales, g)
                residual = jnp.where(keep_of(b, at, LANES), total, 0.0)
                core_in[base, :, lanes_of(skip + g)] = residual
                sums[b] = sums[b] + jnp.sum((residual * residual).reshape(rows // 8, 8, LANES), axis=0)
        return sums

    def update_of(kind, half, skip):
        for b in range(2):
            base = (steps - 2 - first_big + half) * 2 + b
            for g in range(widths[kind] // LANES):
                at = pl.multiple_of(half * big + (skip + g) * LANES, LANES)
                wide = amp[b, :, pl.ds(at, LANES)].astype(jnp.float32)
                new = wide - core_in[base, :, lanes_of(skip + g)] / (gap_of(b, at) + LEVEL_SHIFT)
                out_ref[b, :, pl.ds(at, LANES)] = new.astype(jnp.bfloat16)

    def finish_head(half, sums):
        sums = residual_of(HEAD, half, 0, list(sums))
        update_of(HEAD, half, 0)
        return sums

    lax.fori_loop(0, first_big, send_small, 0)
    lax.fori_loop(first_big, first_big + 3, send_whole, 0)
    send_joined(0)
    send_joined(1)
    hole_copy.wait()
    for copy in energy_copies:
        copy.wait()
    for b in range(2):
        occ_wide[b] = jnp.broadcast_to(occ_energy_ref[b : b + 1, :], (LANES, rows)).T
    lax.fori_loop(steps - 2, steps, keep_base, 0)
    lax.fori_loop(0, 2, settle, 0)
    head = widths[HEAD] // LANES
    sums = [jnp.zeros((8, LANES), jnp.float32)] * 2
    for b in range(2):
        counts_ref[b] = jnp.full((8, LANES), (live_rows[b] * live_cols[b]).astype(jnp.float32), jnp.float32)
    sums = finish_head(0, sums)
    sums = residual_of(LAST, 0, head, sums)
    update_of(LAST, 0, head)
    sums = finish_head(1, sums)
    sums = residual_of(LAST, 1, head, sums)
    for b in range(2):
        squares[b] = sums[b]
        squares_in[me, b] = sums[b]
    for index in range(1, 8):
        square_copy(index, me, peer(index)).start()
    update_of(LAST, 1, head)
    for kind in range(4):
        for at in range(outs[kind].shape[0]):
            link_copy(kind, at, across_x).wait_send()
    for b in range(2):
        for step in range(first_big):
            core_copy(step, b, True).wait_send()
        for step in (steps - 2, steps - 1):
            core_copy(step, b, False).wait_send()
    for index in range(1, 8):
        square_copy(index, me, peer(index)).wait_send()
    for index in range(1, 8):
        square_copy(index, square_source(index), peer(index)).wait_recv()


def emit_kernel(updated, squares, counts, out_hbm, norm_ref, sem):
    copy = pltpu.make_async_copy(updated, out_hbm, sem)
    copy.start()
    for b in range(2):
        total = squares[0, b]
        for index in range(1, squares.shape[0]):
            total = total + squares[index, b]
        total = jnp.full((8, LANES), jnp.sum(total), jnp.float32)
        norm_ref[b] = jnp.sqrt(total / counts[b] + EPSILON)[0, 0]
    copy.wait()


def group_body(amplitudes, ladder_ints, hole_ints, occ_energy, vir_energy, occ_pairs, vir_pairs):
    blocks, rows, cols = amplitudes.shape
    big = cols // 2
    small = big // 3
    units = ((6, small), (6, big), (4, big - small), (4, small))
    coded = [pltpu.VMEM((count, width // LANES * rows + CODE_ROWS, LANES), jnp.int16) for count, width in units]
    anywhere = pl.BlockSpec(memory_space=pl.ANY)
    vmem = pl.BlockSpec(memory_space=pltpu.VMEM)
    smem = pl.BlockSpec(memory_space=pltpu.SMEM)
    dma = pltpu.SemaphoreType.DMA
    sems = [dma((count,)) for count, _ in units]
    outs = pl.pallas_call(
        functools.partial(group_kernel, (rows, cols)),
        in_specs=[anywhere] * 7,
        out_specs=[vmem] * 3,
        out_shape=[
            pltpu.VMEM((blocks, rows, cols), jnp.bfloat16),
            pltpu.VMEM((8, blocks, 8, LANES), jnp.float32),
            pltpu.VMEM((blocks, 8, LANES), jnp.float32),
        ],
        scratch_shapes=[
            pltpu.VMEM((2, rows, cols), jnp.bfloat16),
            pltpu.VMEM((2, rows, rows), jnp.bfloat16),
            pltpu.VMEM((2, rows, LANES), jnp.float32),
            pltpu.VMEM((6, cols, big), jnp.bfloat16),
            pltpu.VMEM((6, rows, small), jnp.float32),
            pltpu.VMEM((4, rows, big), jnp.float32),
            pltpu.VMEM((6, rows, small), jnp.float32),
            pltpu.VMEM((14, rows, big), jnp.float32),
            pltpu.VMEM((2, rows, big), jnp.float32),
            pltpu.VMEM((2, 8, LANES), jnp.float32),
            pltpu.SMEM(occ_pairs.shape, jnp.int32),
            pltpu.SMEM(vir_pairs.shape, jnp.int32),
            pltpu.VMEM(occ_energy.shape, jnp.float32),
            pltpu.VMEM(vir_energy.shape, jnp.float32),
            dma((2,)), dma((2,)),
            dma((2,)), dma(()), dma((6,)), dma((6,)), dma((4,)), dma((6,)), dma((14,)), dma((7,)), dma((8,)),
            *coded, *coded, *sems, *sems,
        ],
        compiler_params=pltpu.CompilerParams(
            collective_id=0, has_side_effects=True, vmem_limit_bytes=VMEM_BYTES
        ),
        name="ladder_group",
    )(occ_pairs, vir_pairs, amplitudes, ladder_ints, hole_ints, occ_energy, vir_energy)
    return pl.pallas_call(
        emit_kernel,
        in_specs=[vmem] * 3,
        out_specs=[anywhere, smem],
        out_shape=[
            jax.ShapeDtypeStruct((blocks, rows, cols), jnp.bfloat16),
            jax.ShapeDtypeStruct((blocks,), jnp.float32),
        ],
        scratch_shapes=[dma(())],
        compiler_params=pltpu.CompilerParams(vmem_limit_bytes=2**20),
        name="emit",
    )(*outs)


def solution(mesh):
    in_specs = (
        P("irrep", None, SLOTS),
        P("irrep", SLOTS, None),
        P("irrep", None, None),
        P("irrep", None),
        P("irrep", SLOTS),
        P(),
        P(),
    )
    out_specs = (P("irrep", None, SLOTS), P("irrep"))

    def chosen(amplitudes, *rest):
        return (group_body if fits_group(mesh, amplitudes.shape[2]) else body)(amplitudes, *rest)

    return jax.shard_map(chosen, mesh=mesh, in_specs=in_specs, out_specs=out_specs, check_vma=False)
```

```python
import functools

import jax
import jax.numpy as jnp
from jax import lax
from jax.experimental import pallas as pl
from jax.experimental.pallas import tpu as pltpu
from jax.sharding import PartitionSpec as P

LEVEL_SHIFT = 0.5
EPSILON = 1e-06
GRID_STEPS = 256.0
TOP = 32767.0
CODE_ROWS = 16
HALF_TILE = 8
BANDS = 2
SLOTS = ("occ", "vir")
LANES = 128
VMEM_BYTES = 58 * 2**20
MESH = pl.DeviceIdType.MESH


def encode(value, out_ref):
    rows, cols = value.shape
    largest = jnp.max(jnp.abs(value), axis=0, keepdims=True)
    code = jnp.ceil(jnp.log2(jnp.maximum(largest, 1e-30)) * GRID_STEPS) + 1.0
    scaled = value * (jnp.exp2(code * (-1.0 / GRID_STEPS)) * TOP)
    out_ref[0:rows, :] = jnp.round(scaled).astype(jnp.int32).astype(jnp.int16)
    out_ref[rows : rows + CODE_ROWS, :] = (
        jnp.broadcast_to(code, (CODE_ROWS, cols)).astype(jnp.int32).astype(jnp.int16)
    )


def decode(in_ref):
    rows = in_ref.shape[0] - CODE_ROWS
    codes = in_ref[rows : rows + CODE_ROWS, :].astype(jnp.int32).astype(jnp.float32)
    scale = jnp.exp2(codes[0:1, :] * (1.0 / GRID_STEPS)) * (1.0 / TOP)
    return in_ref[0:rows, :].astype(jnp.int32).astype(jnp.float32) * scale


def ladder_kernel(received, coded, slot_ref, amp_ref, ladder_ref, *refs):
    out_ref = refs[-1]
    value = jnp.dot(amp_ref[0], ladder_ref[0], preferred_element_type=jnp.float32)
    for ref in refs[:received]:
        value = value + decode(ref)
    if coded:
        encode(value, out_ref)
    else:
        out_ref[...] = value


def tile_of(cols):
    return next(size for size in (768, 512, 384, 256, 128) if cols % size == 0)


def ladder_call(block, slot, masked, ladder, received, coded):
    _, rows, cols = masked.shape
    tile = tile_of(cols)
    steps = cols // tile
    out_rows, out_type = (rows + CODE_ROWS, jnp.int16) if coded else (rows, jnp.float32)
    return pl.pallas_call(
        functools.partial(ladder_kernel, len(received), coded),
        grid_spec=pltpu.PrefetchScalarGridSpec(
            num_scalar_prefetch=1,
            grid=(steps,),
            in_specs=[
                pl.BlockSpec((1, rows, cols), lambda j, slot: (block, 0, 0)),
                pl.BlockSpec((1, cols, tile), lambda j, slot: (block, 0, slot[0] * steps + j)),
            ]
            + [pl.BlockSpec((rows + CODE_ROWS, tile), lambda j, slot: (0, j))] * len(received),
            out_specs=pl.BlockSpec((out_rows, tile), lambda j, slot: (0, j)),
        ),
        out_shape=jax.ShapeDtypeStruct((out_rows, cols), out_type),
        cost_estimate=pl.CostEstimate(
            flops=2 * rows * cols * cols,
            bytes_accessed=2 * cols * cols + 4 * rows * cols * (1 + len(received)),
            transcendentals=0,
        ),
        name="ladder",
    )(slot.reshape(1), masked, ladder, *received)


def join_kernel(total_ref, *refs):
    value = total_ref[...]
    for ref in refs[:-1]:
        value = value + decode(ref)
    encode(value, refs[-1])


def join_call(total, received):
    rows, cols = total.shape
    tile = tile_of(cols)
    coded = pl.BlockSpec((rows + CODE_ROWS, tile), lambda j: (0, j))
    return pl.pallas_call(
        join_kernel,
        grid=(cols // tile,),
        in_specs=[pl.BlockSpec((rows, tile), lambda j: (0, j))] + [coded] * len(received),
        out_specs=coded,
        out_shape=jax.ShapeDtypeStruct((rows + CODE_ROWS, cols), jnp.int16),
        cost_estimate=pl.CostEstimate(
            flops=8 * rows * cols, bytes_accessed=(6 + 2 * len(received)) * rows * cols, transcendentals=0
        ),
        name="join",
    )(total, *received)


def final_kernel(blocks, parts, start_ref, occ_ref, vir_ref, amp_ref, hole_ref, occ_energy_ref, vir_energy_ref, *refs):
    out_ref, square_ref = refs[-2], refs[-1]
    rows, tile = out_ref.shape[1:]
    step = pl.program_id(0)
    column = start_ref[0] + step * tile + lax.broadcasted_iota(jnp.int32, (rows, tile), 1)
    row = lax.broadcasted_iota(jnp.int32, (rows, tile), 0)
    for block in range(blocks):
        mine = refs[block * parts : (block + 1) * parts]
        value = mine[0][...]
        for ref in mine[1:]:
            value = value + decode(ref)
        amp = amp_ref[block]
        value = value + jnp.dot(hole_ref[block], amp, preferred_element_type=jnp.float32)
        wide = amp.astype(jnp.float32)
        denominator = vir_energy_ref[block] - occ_energy_ref[block]
        keep = (row < occ_ref[block]) & (column < vir_ref[block])
        residual = jnp.where(keep, value + denominator * wide, 0.0)
        out_ref[block] = (wide - residual / (denominator + LEVEL_SHIFT)).astype(jnp.bfloat16)
        squares = jnp.sum((residual * residual).reshape(rows // 8, 8, tile), axis=0)
        squares = jnp.broadcast_to(jnp.sum(squares), (8, 128))

        @pl.when(step == 0)
        def _():
            square_ref[block] = squares

        @pl.when(step != 0)
        def _():
            square_ref[block] += squares


def final_call(start, occ_here, vir_here, masked, hole, occ_energy, vir_energy, operands):
    blocks, rows, cols = masked.shape
    parts = len(operands[0])
    tile = 512 if cols % 512 == 0 else tile_of(cols)
    total = pl.BlockSpec((rows, tile), lambda j, *_: (0, j))
    coded = pl.BlockSpec((rows + CODE_ROWS, tile), lambda j, *_: (0, j))
    return pl.pallas_call(
        functools.partial(final_kernel, blocks, parts),
        grid_spec=pltpu.PrefetchScalarGridSpec(
            num_scalar_prefetch=3,
            grid=(cols // tile,),
            in_specs=[
                pl.BlockSpec((blocks, rows, tile), lambda j, *_: (0, 0, j)),
                pl.BlockSpec((blocks, rows, rows), lambda j, *_: (0, 0, 0)),
                pl.BlockSpec((blocks, rows, 1), lambda j, *_: (0, 0, 0)),
                pl.BlockSpec((blocks, 1, tile), lambda j, *_: (0, 0, j)),
            ]
            + ([total] + [coded] * (parts - 1)) * blocks,
            out_specs=[
                pl.BlockSpec((blocks, rows, tile), lambda j, *_: (0, 0, j)),
                pl.BlockSpec((blocks, 8, 128), lambda j, *_: (0, 0, 0)),
            ],
        ),
        out_shape=[
            jax.ShapeDtypeStruct((blocks, rows, cols), jnp.bfloat16),
            jax.ShapeDtypeStruct((blocks, 8, 128), jnp.float32),
        ],
        cost_estimate=pl.CostEstimate(
            flops=2 * blocks * rows * rows * cols, bytes_accessed=12 * blocks * rows * cols, transcendentals=0
        ),
        name="final",
    )(
        start.reshape(1), occ_here, vir_here, masked, hole,
        occ_energy[:, :, None], vir_energy[:, None, :], *[x for group in operands for x in group],
    )


def table_lookup(table, block_ids):
    entries = table.shape[0]
    match = jnp.arange(entries, dtype=jnp.int32)[None, :] == block_ids[:, None]
    return jnp.sum(jnp.where(match, table[None, :], 0), axis=1)


def body(amplitudes, ladder_ints, hole_ints, occ_energy, vir_energy, occ_pairs, vir_pairs):
    blocks, rows, cols = amplitudes.shape
    occ_size, vir_size = lax.axis_size("occ"), lax.axis_size("vir")
    slots = occ_size * vir_size
    block_ids = lax.axis_index("irrep") * blocks + jnp.arange(blocks, dtype=jnp.int32)
    slot = lax.axis_index("occ") * vir_size + lax.axis_index("vir")
    start = slot * cols
    occ_here = table_lookup(occ_pairs, block_ids)
    vir_here = table_lookup(vir_pairs, block_ids)
    row = jnp.arange(rows, dtype=jnp.int32)
    column = start + jnp.arange(cols, dtype=jnp.int32)
    keep = (row[None, :, None] < occ_here[:, None, None]) & (column[None, None, :] < vir_here[:, None, None])
    masked = jnp.where(keep, amplitudes, jnp.zeros((), amplitudes.dtype))

    core = vir_size if occ_size > vir_size else 1
    bits = [1 << i for i in range(slots.bit_length() - 1) if 1 << i != core]

    def exchange(array, bit):
        return lax.ppermute(array, SLOTS, [(s, s ^ bit) for s in range(slots)])

    orders = [bits if block % 2 == 0 else bits[::-1] for block in range(blocks)]
    arrived = [{} for _ in range(blocks)]
    for rank in range((1 << len(bits)) - 1, -1, -1):
        chosen = [i for i in range(len(bits)) if rank >> (len(bits) - 1 - i) & 1]
        flips = [sum(order[i] for i in chosen) for order in orders]
        firsts = [ladder_call(b, slot ^ (flips[b] | core), masked, ladder_ints, [], True) for b in range(blocks)]
        firsts = [exchange(first, core) for first in firsts]
        for b in range(blocks):
            order, got = orders[b], arrived[b].get(flips[b], [])
            direct = bool(chosen) and not got
            total = ladder_call(b, slot ^ flips[b], masked, ladder_ints, [firsts[b]], direct)
            if not chosen:
                arrived[b][0] = [total] + got
                continue
            packed = total if direct else join_call(total, got)
            bit = order[chosen[0]]
            arrived[b].setdefault(flips[b] ^ bit, []).append(exchange(packed, bit))
    updated, squares = final_call(
        start, occ_here, vir_here, masked, hole_ints, occ_energy, vir_energy, [arrived[b][0] for b in range(blocks)]
    )
    summed_squares = lax.psum(squares[:, 0, 0], SLOTS)
    pair_count = (occ_here * vir_here).astype(jnp.float32)
    return updated, jnp.sqrt(summed_squares / pair_count + EPSILON)


def fits_group(mesh, cols):
    return mesh.shape["occ"] == 4 and mesh.shape["vir"] == 2 and cols % (6 * LANES) == 0


def group_kernel(
    dims, occ_hbm, vir_hbm, amp_hbm, ladder_hbm, hole_hbm, occ_energy_hbm, vir_energy_hbm, out_ref, squares_in, counts_ref,
    amp, hole, occ_wide, lad, parts_small, parts, core_in_small, core_in, squares,
    occ_ref, vir_ref, occ_energy_ref, vir_energy_ref, pair_sem, energy_sem,
    amp_sem, hole_sem, lad_sem, core_send_small, core_send, core_recv_small, core_recv, square_send, square_recv, *links,
):
    rows, cols = dims
    big = cols // 2
    small = big // 3
    first_big, steps, lad_slots = 6, 12, lad.shape[0]
    outs, ins, sends, recvs = links[0:4], links[4:8], links[8:12], links[12:16]
    SMALL, WHOLE, HEAD, LAST = range(4)
    widths = (small, big, big - small, small)
    x, o = lax.axis_index("vir"), lax.axis_index("occ")
    y, core = o // 2, o % 2
    me = o * 2 + x
    first = lax.axis_index("irrep") * 2
    across_core = {"occ": o + 1 - 2 * core}

    def near_side(b):
        return {"occ": (o + 2 * b) % 4, "vir": (x + 1 - b) % 2}

    def far_side(b):
        return near_side(1 - b)

    def twice(one):
        lax.fori_loop(0, 2, lambda b, carry: (one(b), carry)[1], 0)


    def remote(src, dst, send, recv, target):
        return pltpu.make_async_remote_copy(
            src_ref=src, dst_ref=dst, send_sem=send, recv_sem=recv, device_id=target, device_id_type=MESH
        )

    def lad_copy(step, k, is_small):
        b, role = k % 2, k // 2
        half = step - first_big + 2
        phase = 0 if is_small else half // 2
        column = step * small if is_small else (half % 2) * big
        upper, lower = 1 - phase // 2, 1 - phase % 2
        flip_x, flip_y = upper * (1 - b) + lower * b, lower * (1 - b) + upper * b
        target_core = (core + 1 - role) % 2
        target = (((y + flip_y) % 2) * 2 + target_core) * 2 + (x + flip_x) % 2
        slot = (4 * step + k) % lad_slots
        width = small if is_small else big
        source = ladder_hbm.at[b, :, pl.ds(pl.multiple_of(target * cols + column, LANES), width)]
        return pltpu.make_async_copy(source, lad.at[slot, :, pl.ds(0, width)], lad_sem.at[slot])

    def core_copy(step, b, is_small):
        if is_small:
            at = step * 2 + b
            return remote(parts_small.at[at], core_in_small.at[at], core_send_small.at[at], core_recv_small.at[at], across_core)
        slot, at = (step % 2) * 2 + b, (step - first_big) * 2 + b
        return remote(parts.at[slot], core_in.at[at], core_send.at[slot], core_recv.at[at], across_core)

    def link_copy(kind, at, target):
        return remote(outs[kind].at[at], ins[kind].at[at], sends[kind].at[at], recvs[kind].at[at], target)

    def square_copy(index, sender, target):
        return remote(squares, squares_in.at[sender], square_send.at[index - 1], square_recv.at[sender], target)

    def square_source(index):
        return ((o + 4 - index // 2) % 4) * 2 + (x + index) % 2

    def peer(index):
        return {"occ": (o + index // 2) % 4, "vir": (x + index) % 2}

    def amp_copy(b):
        return pltpu.make_async_copy(amp_hbm.at[b], amp.at[b], amp_sem.at[b])

    hole_copy = pltpu.make_async_copy(hole_hbm, hole, hole_sem)
    pair_copies = [
        pltpu.make_async_copy(occ_hbm, occ_ref, pair_sem.at[0]), pltpu.make_async_copy(vir_hbm, vir_ref, pair_sem.at[1])
    ]
    energy_copies = [
        pltpu.make_async_copy(occ_energy_hbm, occ_energy_ref, energy_sem.at[0]),
        pltpu.make_async_copy(vir_energy_hbm, vir_energy_ref, energy_sem.at[1]),
    ]
    barrier = pltpu.get_barrier_semaphore()
    for index in range(1, 8):
        pl.semaphore_signal(barrier, inc=1, device_id=peer(index), device_id_type=MESH)
    for copy in pair_copies:
        copy.start()
    for b in range(2):
        amp_copy(b).start()
        lad_copy(0, b, True).start()
    for copy in pair_copies:
        copy.wait()

    def keep_of(b, column0, width):
        row = lax.broadcasted_iota(jnp.int32, (rows, width), 0)
        column = me * cols + column0 + lax.broadcasted_iota(jnp.int32, (rows, width), 1)
        return (row < occ_ref[first + b]) & (column < vir_ref[first + b])

    def mask(b):
        amp_copy(b).wait()
        shape = (16, LANES)
        lane = me * cols + lax.broadcasted_iota(jnp.int32, shape, 1)
        masks = [
            jnp.where(lane + g * LANES < vir_ref[first + b], 1.0, 0.0).astype(jnp.bfloat16) for g in range(cols // LANES)
        ]

        def one(index, carry):
            row0 = pl.multiple_of(index * 16, 16)
            row = row0 + lax.broadcasted_iota(jnp.int32, shape, 0)
            live = jnp.where(row < occ_ref[first + b], 1.0, 0.0).astype(jnp.bfloat16)
            for g in range(cols // LANES):
                lanes = slice(g * LANES, (g + 1) * LANES)
                amp[b, pl.ds(row0, 16), lanes] = amp[b, pl.ds(row0, 16), lanes] * masks[g] * live
            return carry

        lax.fori_loop(0, rows // 16, one, 0)

    for n in range(2, lad_slots):
        lad_copy(n // 4, n % 4, True).start()
    hole_copy.start()
    for copy in energy_copies:
        copy.start()
    twice(mask)
    pl.semaphore_wait(barrier, 7)

    def part(step, k, is_small):
        lad_copy(step, k, is_small).wait()
        width = small if is_small else big
        return jnp.dot(amp[k % 2], lad[(4 * step + k) % lad_slots, :, 0:width], preferred_element_type=jnp.float32)

    def refill(step, k, is_small):
        ahead = 4 * step + k + lad_slots
        later, k_later = step + (k + lad_slots) // 4, (k + lad_slots) % 4
        if is_small:

            @pl.when(later < first_big)
            def _():
                lad_copy(later, k_later, True).start()

            @pl.when(later >= first_big)
            def _():
                lad_copy(later, k_later, False).start()
        else:

            @pl.when(later < steps)
            def _():
                lad_copy(later, k_later, False).start()

    def produce(step, is_small):
        target, spare = (parts_small, 2 * first_big) if is_small else (parts, 4)

        def one(k, carry):
            b, theirs = k % 2, k < 2
            if not is_small:

                @pl.when(theirs & (step >= first_big + 2))
                def _():
                    core_copy(step - 2, b, False).wait_send()

            given = step * 2 + b if is_small else (step % 2) * 2 + b
            target[jnp.where(theirs, given, spare + b)] = part(step, k, is_small)

            @pl.when(theirs)
            def _():
                core_copy(step, b, is_small).start()

            refill(step, k, is_small)
            return carry

        lax.fori_loop(0, 4, one, 0)

    def lanes_of(g):
        return slice(g * LANES, (g + 1) * LANES)

    def both_cores(step, b, g, is_small):
        source, at = (core_in_small, step * 2 + b) if is_small else (core_in, (step - first_big) * 2 + b)
        own, slot = (parts_small, 2 * first_big + b) if is_small else (parts, 4 + b)
        return own[slot, :, lanes_of(g)] + source[at, :, lanes_of(g)]

    def scales_of(kind, at):
        top = widths[kind] // LANES * rows
        codes = ins[kind][at, top : top + HALF_TILE, :].astype(jnp.int32).astype(jnp.float32)
        return jnp.exp2(codes * (1.0 / GRID_STEPS)) * (1.0 / TOP)

    def decoded(kind, at, scales, g):
        return ins[kind][at, g * rows : (g + 1) * rows, :].astype(jnp.int32).astype(jnp.float32) * scales[g : g + 1, :]

    def send(kind, at, values, target):
        out = outs[kind]
        codes = jnp.zeros((HALF_TILE, LANES), jnp.float32)
        which = lax.broadcasted_iota(jnp.int32, (HALF_TILE, LANES), 0)
        groups = widths[kind] // LANES
        for g in range(groups):
            value = values(g)
            largest = jnp.max(jnp.abs(value), axis=0, keepdims=True)
            code = jnp.ceil(jnp.log2(jnp.maximum(largest, 1e-30)) * GRID_STEPS) + 1.0
            scaled = value * (jnp.exp2(code * (-1.0 / GRID_STEPS)) * TOP)
            out[at, g * rows : (g + 1) * rows, :] = jnp.round(scaled).astype(jnp.int32).astype(jnp.int16)
            codes = jnp.where(which == g, jnp.broadcast_to(code, (HALF_TILE, LANES)), codes)
        out[at, groups * rows : groups * rows + HALF_TILE, :] = codes.astype(jnp.int32).astype(jnp.int16)
        link_copy(kind, at, target).start()

    def send_small(step, carry):
        produce(step, True)

        def one(b):
            core_copy(step, b, True).wait_recv()
            send(SMALL, step * 2 + b, lambda g: both_cores(step, b, g, True), near_side(b))

        twice(one)
        return carry

    def send_whole(step, carry):
        produce(step, False)

        def one(b):
            core_copy(step, b, False).wait_recv()
            at = (step - first_big) * 2 + b
            send(WHOLE, at, lambda g: both_cores(step, b, g, False), near_side(b))

        twice(one)
        return carry

    def send_joined(half, carry):
        step = first_big + 2 + half
        produce(step, False)

        def one(b):
            core_copy(step, b, False).wait_recv()
            arrived = []
            for piece in range(3):
                at = 2 * (half * 3 + piece) + b
                link_copy(SMALL, at, near_side(b)).wait_recv()
                scales = scales_of(SMALL, at)
                arrived += [(SMALL, at, scales, g) for g in range(small // LANES)]

            def value(g):
                return both_cores(step, b, g, False) + decoded(*arrived[g])

            head = widths[HEAD] // LANES
            send(HEAD, half * 2 + b, value, far_side(b))
            send(LAST, half * 2 + b, lambda g: value(head + g), far_side(b))

        twice(one)
        return carry

    def gap_of(b, column):
        both = vir_energy_ref[:, pl.ds(column, LANES)]
        return jnp.where(b == 0, both[0:1], both[1:2]) - occ_wide[b]

    def keep_base(step, carry):
        produce(step, False)
        start = (step - (steps - 2)) * big

        def one(b):
            from_hole = jnp.dot(
                hole[b], amp[b, :, pl.ds(pl.multiple_of(start, LANES), big)], preferred_element_type=jnp.float32
            )
            core_copy(step, b, False).wait_recv()
            for g in range(big // LANES):
                at = pl.multiple_of(start + g * LANES, LANES)
                wide = amp[b, :, pl.ds(at, LANES)].astype(jnp.float32)
                total = both_cores(step, b, g, False) + from_hole[:, lanes_of(g)] + gap_of(b, at) * wide
                core_in[(step - first_big) * 2 + b, :, lanes_of(g)] = total

        twice(one)
        return carry

    def settle(half, carry):
        def one(b):
            at = half * 2 + b
            link_copy(WHOLE, at, near_side(b)).wait_recv()
            scales = scales_of(WHOLE, at)
            base = (steps - 2 - first_big + half) * 2 + b
            for g in range(big // LANES):
                core_in[base, :, lanes_of(g)] = core_in[base, :, lanes_of(g)] + decoded(WHOLE, at, scales, g)

        twice(one)
        return carry

    def residual_of(kind, half, skip):
        def one(b):
            link_copy(kind, half * 2 + b, far_side(b)).wait_recv()
            scales = scales_of(kind, half * 2 + b)
            base = (steps - 2 - first_big + half) * 2 + b
            for g in range(widths[kind] // LANES):
                at = pl.multiple_of(half * big + (skip + g) * LANES, LANES)
                total = core_in[base, :, lanes_of(skip + g)] + decoded(kind, half * 2 + b, scales, g)
                residual = jnp.where(keep_of(b, at, LANES), total, 0.0)
                core_in[base, :, lanes_of(skip + g)] = residual
                squares[b] = squares[b] + jnp.sum((residual * residual).reshape(rows // 8, 8, LANES), axis=0)

        twice(one)

    def update_of(kind, half, skip):
        def one(b):
            base = (steps - 2 - first_big + half) * 2 + b
            for g in range(widths[kind] // LANES):
                at = pl.multiple_of(half * big + (skip + g) * LANES, LANES)
                wide = amp[b, :, pl.ds(at, LANES)].astype(jnp.float32)
                new = wide - core_in[base, :, lanes_of(skip + g)] / (gap_of(b, at) + LEVEL_SHIFT)
                out_ref[b, :, pl.ds(at, LANES)] = new.astype(jnp.bfloat16)

        twice(one)

    lax.fori_loop(0, first_big, send_small, 0)
    lax.fori_loop(first_big, first_big + 2, send_whole, 0)
    lax.fori_loop(0, 2, send_joined, 0)
    hole_copy.wait()
    for copy in energy_copies:
        copy.wait()
    for b in range(2):
        occ_wide[b] = jnp.broadcast_to(occ_energy_ref[b : b + 1, :], (LANES, rows)).T
    lax.fori_loop(steps - 2, steps, keep_base, 0)
    lax.fori_loop(0, 2, settle, 0)
    head = widths[HEAD] // LANES
    for b in range(2):
        squares[b] = jnp.zeros((8, LANES), jnp.float32)
        counts_ref[b] = jnp.full((8, LANES), (occ_ref[first + b] * vir_ref[first + b]).astype(jnp.float32), jnp.float32)

    def finish(half, carry):
        residual_of(HEAD, half, 0)
        update_of(HEAD, half, 0)
        residual_of(LAST, half, head)

        @pl.when(half == 0)
        def _():
            update_of(LAST, half, head)

        return carry

    lax.fori_loop(0, 2, finish, 0)
    squares_in[me] = squares[...]
    for index in range(1, 8):
        square_copy(index, me, peer(index)).start()
    update_of(LAST, 1, head)
    for kind in range(4):
        for at in range(outs[kind].shape[0]):
            link_copy(kind, at, near_side(0)).wait_send()
    for b in range(2):
        for step in range(first_big):
            core_copy(step, b, True).wait_send()
        for step in (steps - 2, steps - 1):
            core_copy(step, b, False).wait_send()
    for index in range(1, 8):
        square_copy(index, me, peer(index)).wait_send()
    for index in range(1, 8):
        square_copy(index, square_source(index), peer(index)).wait_recv()


def emit_kernel(updated, squares, counts, out_hbm, norm_hbm, norm_ref, norm_sem, sem):
    band = updated.shape[1] // BANDS
    copies = [
        pltpu.make_async_copy(updated.at[b, pl.ds(i * band, band)], out_hbm.at[b, pl.ds(i * band, band)], sem.at[b * BANDS + i])
        for b in range(2)
        for i in range(BANDS)
    ]
    for copy in copies:
        copy.start()
    for b in range(2):
        total = squares[0, b]
        for index in range(1, squares.shape[0]):
            total = total + squares[index, b]
        total = jnp.full((8, LANES), jnp.sum(total), jnp.float32)
        norm_ref[b] = jnp.sqrt(total / counts[b] + EPSILON)[0, 0]
    copies.append(pltpu.make_async_copy(norm_ref, norm_hbm, norm_sem))
    copies[-1].start()
    for copy in copies:
        copy.wait()


def group_body(amplitudes, ladder_ints, hole_ints, occ_energy, vir_energy, occ_pairs, vir_pairs):
    blocks, rows, cols = amplitudes.shape
    big = cols // 2
    small = big // 3
    units = ((12, small), (4, big), (4, big - small), (4, small))
    coded = [pltpu.VMEM((count, width // LANES * rows + HALF_TILE, LANES), jnp.int16) for count, width in units]
    anywhere = pl.BlockSpec(memory_space=pl.ANY)
    vmem = pl.BlockSpec(memory_space=pltpu.VMEM)
    smem = pl.BlockSpec(memory_space=pltpu.SMEM)
    dma = pltpu.SemaphoreType.DMA
    sems = [dma((count,)) for count, _ in units]
    outs = pl.pallas_call(
        functools.partial(group_kernel, (rows, cols)),
        in_specs=[anywhere] * 7,
        out_specs=[vmem] * 3,
        out_shape=[
            pltpu.VMEM((blocks, rows, cols), jnp.bfloat16),
            pltpu.VMEM((8, blocks, 8, LANES), jnp.float32),
            pltpu.VMEM((blocks, 8, LANES), jnp.float32),
        ],
        scratch_shapes=[
            pltpu.VMEM((2, rows, cols), jnp.bfloat16),
            pltpu.VMEM((2, rows, rows), jnp.bfloat16),
            pltpu.VMEM((2, rows, LANES), jnp.float32),
            pltpu.VMEM((6, cols, big), jnp.bfloat16),
            pltpu.VMEM((14, rows, small), jnp.float32),
            pltpu.VMEM((6, rows, big), jnp.float32),
            pltpu.VMEM((12, rows, small), jnp.float32),
            pltpu.VMEM((12, rows, big), jnp.float32),
            pltpu.VMEM((2, 8, LANES), jnp.float32),
            pltpu.SMEM(occ_pairs.shape, jnp.int32),
            pltpu.SMEM(vir_pairs.shape, jnp.int32),
            pltpu.VMEM(occ_energy.shape, jnp.float32),
            pltpu.VMEM(vir_energy.shape, jnp.float32),
            dma((2,)), dma((2,)),
            dma((2,)), dma(()), dma((6,)), dma((12,)), dma((4,)), dma((12,)), dma((12,)), dma((7,)), dma((8,)),
            *coded, *coded, *sems, *sems,
        ],
        compiler_params=pltpu.CompilerParams(
            collective_id=0, has_side_effects=True, vmem_limit_bytes=VMEM_BYTES
        ),
        name="ladder_group",
    )(occ_pairs, vir_pairs, amplitudes, ladder_ints, hole_ints, occ_energy, vir_energy)
    return pl.pallas_call(
        emit_kernel,
        in_specs=[vmem] * 3,
        out_specs=[anywhere] * 2,
        out_shape=[
            jax.ShapeDtypeStruct((blocks, rows, cols), jnp.bfloat16),
            jax.ShapeDtypeStruct((blocks,), jnp.float32),
        ],
        scratch_shapes=[pltpu.SMEM((blocks,), jnp.float32), dma(()), dma((2 * BANDS,))],
        compiler_params=pltpu.CompilerParams(vmem_limit_bytes=2**20),
        name="emit",
    )(*outs)


def solution(mesh):
    in_specs = (
        P("irrep", None, SLOTS),
        P("irrep", SLOTS, None),
        P("irrep", None, None),
        P("irrep", None),
        P("irrep", SLOTS),
        P(),
        P(),
    )
    out_specs = (P("irrep", None, SLOTS), P("irrep"))

    def chosen(amplitudes, *rest):
        return (group_body if fits_group(mesh, amplitudes.shape[2]) else body)(amplitudes, *rest)

    return jax.shard_map(chosen, mesh=mesh, in_specs=in_specs, out_specs=out_specs, check_vma=False)
```

```python
import functools

import jax
import jax.numpy as jnp
from jax import lax
from jax.experimental import pallas as pl
from jax.experimental.pallas import tpu as pltpu
from jax.sharding import PartitionSpec as P

LEVEL_SHIFT = 0.5
EPSILON = 1e-06
GRID_STEPS = 256.0
TOP = 32767.0
CODE_ROWS = 16
HALF_TILE = 8
BANDS = 2
SLOTS = ("occ", "vir")
LANES = 128
VMEM_BYTES = 58 * 2**20
MESH = pl.DeviceIdType.MESH


def encode(value, out_ref):
    rows, cols = value.shape
    largest = jnp.max(jnp.abs(value), axis=0, keepdims=True)
    code = jnp.ceil(jnp.log2(jnp.maximum(largest, 1e-30)) * GRID_STEPS) + 1.0
    scaled = value * (jnp.exp2(code * (-1.0 / GRID_STEPS)) * TOP)
    out_ref[0:rows, :] = jnp.round(scaled).astype(jnp.int32).astype(jnp.int16)
    out_ref[rows : rows + CODE_ROWS, :] = (
        jnp.broadcast_to(code, (CODE_ROWS, cols)).astype(jnp.int32).astype(jnp.int16)
    )


def decode(in_ref):
    rows = in_ref.shape[0] - CODE_ROWS
    codes = in_ref[rows : rows + CODE_ROWS, :].astype(jnp.int32).astype(jnp.float32)
    scale = jnp.exp2(codes[0:1, :] * (1.0 / GRID_STEPS)) * (1.0 / TOP)
    return in_ref[0:rows, :].astype(jnp.int32).astype(jnp.float32) * scale


def ladder_kernel(received, coded, slot_ref, amp_ref, ladder_ref, *refs):
    out_ref = refs[-1]
    value = jnp.dot(amp_ref[0], ladder_ref[0], preferred_element_type=jnp.float32)
    for ref in refs[:received]:
        value = value + decode(ref)
    if coded:
        encode(value, out_ref)
    else:
        out_ref[...] = value


def tile_of(cols):
    return next(size for size in (768, 512, 384, 256, 128) if cols % size == 0)


def ladder_call(block, slot, masked, ladder, received, coded):
    _, rows, cols = masked.shape
    tile = tile_of(cols)
    steps = cols // tile
    out_rows, out_type = (rows + CODE_ROWS, jnp.int16) if coded else (rows, jnp.float32)
    return pl.pallas_call(
        functools.partial(ladder_kernel, len(received), coded),
        grid_spec=pltpu.PrefetchScalarGridSpec(
            num_scalar_prefetch=1,
            grid=(steps,),
            in_specs=[
                pl.BlockSpec((1, rows, cols), lambda j, slot: (block, 0, 0)),
                pl.BlockSpec((1, cols, tile), lambda j, slot: (block, 0, slot[0] * steps + j)),
            ]
            + [pl.BlockSpec((rows + CODE_ROWS, tile), lambda j, slot: (0, j))] * len(received),
            out_specs=pl.BlockSpec((out_rows, tile), lambda j, slot: (0, j)),
        ),
        out_shape=jax.ShapeDtypeStruct((out_rows, cols), out_type),
        cost_estimate=pl.CostEstimate(
            flops=2 * rows * cols * cols,
            bytes_accessed=2 * cols * cols + 4 * rows * cols * (1 + len(received)),
            transcendentals=0,
        ),
        name="ladder",
    )(slot.reshape(1), masked, ladder, *received)


def join_kernel(total_ref, *refs):
    value = total_ref[...]
    for ref in refs[:-1]:
        value = value + decode(ref)
    encode(value, refs[-1])


def join_call(total, received):
    rows, cols = total.shape
    tile = tile_of(cols)
    coded = pl.BlockSpec((rows + CODE_ROWS, tile), lambda j: (0, j))
    return pl.pallas_call(
        join_kernel,
        grid=(cols // tile,),
        in_specs=[pl.BlockSpec((rows, tile), lambda j: (0, j))] + [coded] * len(received),
        out_specs=coded,
        out_shape=jax.ShapeDtypeStruct((rows + CODE_ROWS, cols), jnp.int16),
        cost_estimate=pl.CostEstimate(
            flops=8 * rows * cols, bytes_accessed=(6 + 2 * len(received)) * rows * cols, transcendentals=0
        ),
        name="join",
    )(total, *received)


def final_kernel(blocks, parts, start_ref, occ_ref, vir_ref, amp_ref, hole_ref, occ_energy_ref, vir_energy_ref, *refs):
    out_ref, square_ref = refs[-2], refs[-1]
    rows, tile = out_ref.shape[1:]
    step = pl.program_id(0)
    column = start_ref[0] + step * tile + lax.broadcasted_iota(jnp.int32, (rows, tile), 1)
    row = lax.broadcasted_iota(jnp.int32, (rows, tile), 0)
    for block in range(blocks):
        mine = refs[block * parts : (block + 1) * parts]
        value = mine[0][...]
        for ref in mine[1:]:
            value = value + decode(ref)
        amp = amp_ref[block]
        value = value + jnp.dot(hole_ref[block], amp, preferred_element_type=jnp.float32)
        wide = amp.astype(jnp.float32)
        denominator = vir_energy_ref[block] - occ_energy_ref[block]
        keep = (row < occ_ref[block]) & (column < vir_ref[block])
        residual = jnp.where(keep, value + denominator * wide, 0.0)
        out_ref[block] = (wide - residual / (denominator + LEVEL_SHIFT)).astype(jnp.bfloat16)
        squares = jnp.sum((residual * residual).reshape(rows // 8, 8, tile), axis=0)
        squares = jnp.broadcast_to(jnp.sum(squares), (8, 128))

        @pl.when(step == 0)
        def _():
            square_ref[block] = squares

        @pl.when(step != 0)
        def _():
            square_ref[block] += squares


def final_call(start, occ_here, vir_here, masked, hole, occ_energy, vir_energy, operands):
    blocks, rows, cols = masked.shape
    parts = len(operands[0])
    tile = 512 if cols % 512 == 0 else tile_of(cols)
    total = pl.BlockSpec((rows, tile), lambda j, *_: (0, j))
    coded = pl.BlockSpec((rows + CODE_ROWS, tile), lambda j, *_: (0, j))
    return pl.pallas_call(
        functools.partial(final_kernel, blocks, parts),
        grid_spec=pltpu.PrefetchScalarGridSpec(
            num_scalar_prefetch=3,
            grid=(cols // tile,),
            in_specs=[
                pl.BlockSpec((blocks, rows, tile), lambda j, *_: (0, 0, j)),
                pl.BlockSpec((blocks, rows, rows), lambda j, *_: (0, 0, 0)),
                pl.BlockSpec((blocks, rows, 1), lambda j, *_: (0, 0, 0)),
                pl.BlockSpec((blocks, 1, tile), lambda j, *_: (0, 0, j)),
            ]
            + ([total] + [coded] * (parts - 1)) * blocks,
            out_specs=[
                pl.BlockSpec((blocks, rows, tile), lambda j, *_: (0, 0, j)),
                pl.BlockSpec((blocks, 8, 128), lambda j, *_: (0, 0, 0)),
            ],
        ),
        out_shape=[
            jax.ShapeDtypeStruct((blocks, rows, cols), jnp.bfloat16),
            jax.ShapeDtypeStruct((blocks, 8, 128), jnp.float32),
        ],
        cost_estimate=pl.CostEstimate(
            flops=2 * blocks * rows * rows * cols, bytes_accessed=12 * blocks * rows * cols, transcendentals=0
        ),
        name="final",
    )(
        start.reshape(1), occ_here, vir_here, masked, hole,
        occ_energy[:, :, None], vir_energy[:, None, :], *[x for group in operands for x in group],
    )


def table_lookup(table, block_ids):
    entries = table.shape[0]
    match = jnp.arange(entries, dtype=jnp.int32)[None, :] == block_ids[:, None]
    return jnp.sum(jnp.where(match, table[None, :], 0), axis=1)


def body(amplitudes, ladder_ints, hole_ints, occ_energy, vir_energy, occ_pairs, vir_pairs):
    blocks, rows, cols = amplitudes.shape
    occ_size, vir_size = lax.axis_size("occ"), lax.axis_size("vir")
    slots = occ_size * vir_size
    block_ids = lax.axis_index("irrep") * blocks + jnp.arange(blocks, dtype=jnp.int32)
    slot = lax.axis_index("occ") * vir_size + lax.axis_index("vir")
    start = slot * cols
    occ_here = table_lookup(occ_pairs, block_ids)
    vir_here = table_lookup(vir_pairs, block_ids)
    row = jnp.arange(rows, dtype=jnp.int32)
    column = start + jnp.arange(cols, dtype=jnp.int32)
    keep = (row[None, :, None] < occ_here[:, None, None]) & (column[None, None, :] < vir_here[:, None, None])
    masked = jnp.where(keep, amplitudes, jnp.zeros((), amplitudes.dtype))

    core = vir_size if occ_size > vir_size else 1
    bits = [1 << i for i in range(slots.bit_length() - 1) if 1 << i != core]

    def exchange(array, bit):
        return lax.ppermute(array, SLOTS, [(s, s ^ bit) for s in range(slots)])

    orders = [bits if block % 2 == 0 else bits[::-1] for block in range(blocks)]
    arrived = [{} for _ in range(blocks)]
    for rank in range((1 << len(bits)) - 1, -1, -1):
        chosen = [i for i in range(len(bits)) if rank >> (len(bits) - 1 - i) & 1]
        flips = [sum(order[i] for i in chosen) for order in orders]
        firsts = [ladder_call(b, slot ^ (flips[b] | core), masked, ladder_ints, [], True) for b in range(blocks)]
        firsts = [exchange(first, core) for first in firsts]
        for b in range(blocks):
            order, got = orders[b], arrived[b].get(flips[b], [])
            direct = bool(chosen) and not got
            total = ladder_call(b, slot ^ flips[b], masked, ladder_ints, [firsts[b]], direct)
            if not chosen:
                arrived[b][0] = [total] + got
                continue
            packed = total if direct else join_call(total, got)
            bit = order[chosen[0]]
            arrived[b].setdefault(flips[b] ^ bit, []).append(exchange(packed, bit))
    updated, squares = final_call(
        start, occ_here, vir_here, masked, hole_ints, occ_energy, vir_energy, [arrived[b][0] for b in range(blocks)]
    )
    summed_squares = lax.psum(squares[:, 0, 0], SLOTS)
    pair_count = (occ_here * vir_here).astype(jnp.float32)
    return updated, jnp.sqrt(summed_squares / pair_count + EPSILON)


def fits_group(mesh, cols):
    return mesh.shape["occ"] == 4 and mesh.shape["vir"] == 2 and cols % (6 * LANES) == 0


def group_kernel(
    dims, occ_hbm, vir_hbm, amp_hbm, ladder_hbm, hole_hbm, occ_energy_hbm, vir_energy_hbm, out_ref, squares_in, counts_ref,
    amp, hole, occ_wide, lad, parts_small, parts, core_in_small, core_in, squares, flat,
    occ_ref, vir_ref, occ_energy_ref, vir_energy_ref, pair_sem, energy_sem,
    amp_sem, hole_sem, lad_sem, core_send_small, core_send, core_recv_small, core_recv, square_send, square_recv, *links,
):
    rows, cols = dims
    big = cols // 2
    small = big // 3
    first_big, steps, lad_slots = 6, 12, lad.shape[0]
    outs, ins, sends, recvs = links[0:4], links[4:8], links[8:12], links[12:16]
    SMALL, WHOLE, HEAD, LAST = range(4)
    widths = (small, big, big - LANES, LANES)
    x, o = lax.axis_index("vir"), lax.axis_index("occ")
    y, core = o // 2, o % 2
    me = o * 2 + x
    first = lax.axis_index("irrep") * 2
    across_core = {"occ": o + 1 - 2 * core}

    def near_side(b):
        return {"occ": (o + 2 * b) % 4, "vir": (x + 1 - b) % 2}

    def far_side(b):
        return near_side(1 - b)

    def twice(one):
        lax.fori_loop(0, 2, lambda b, carry: (one(b), carry)[1], 0)


    def remote(src, dst, send, recv, target):
        return pltpu.make_async_remote_copy(
            src_ref=src, dst_ref=dst, send_sem=send, recv_sem=recv, device_id=target, device_id_type=MESH
        )

    def lad_copy(step, k, is_small):
        b, role = k % 2, k // 2
        half = step - first_big + 2
        phase = 0 if is_small else half // 2
        column = step * small if is_small else (half % 2) * big
        upper, lower = 1 - phase // 2, 1 - phase % 2
        flip_x, flip_y = upper * (1 - b) + lower * b, lower * (1 - b) + upper * b
        target_core = (core + 1 - role) % 2
        target = (((y + flip_y) % 2) * 2 + target_core) * 2 + (x + flip_x) % 2
        slot = (4 * step + k) % lad_slots
        width = small if is_small else big
        source = ladder_hbm.at[b, :, pl.ds(pl.multiple_of(target * cols + column, LANES), width)]
        return pltpu.make_async_copy(source, lad.at[slot, :, pl.ds(0, width)], lad_sem.at[slot])

    def core_copy(step, b, is_small):
        if is_small:
            at = step * 2 + b
            return remote(parts_small.at[at], core_in_small.at[at], core_send_small.at[at], core_recv_small.at[at], across_core)
        slot, at = (step % 2) * 2 + b, (step - first_big) * 2 + b
        return remote(parts.at[slot], core_in.at[at], core_send.at[slot], core_recv.at[at], across_core)

    def link_copy(kind, at, target):
        return remote(outs[kind].at[at], ins[kind].at[at], sends[kind].at[at], recvs[kind].at[at], target)

    def square_copy(index, sender, target):
        return remote(flat, squares_in.at[sender], square_send.at[index - 1], square_recv.at[sender], target)

    def square_source(index):
        return ((o + 4 - index // 2) % 4) * 2 + (x + index) % 2

    def peer(index):
        return {"occ": (o + index // 2) % 4, "vir": (x + index) % 2}

    def amp_copy(b):
        return pltpu.make_async_copy(amp_hbm.at[b], amp.at[b], amp_sem.at[b])

    hole_copy = pltpu.make_async_copy(hole_hbm, hole, hole_sem)
    pair_copies = [
        pltpu.make_async_copy(occ_hbm, occ_ref, pair_sem.at[0]), pltpu.make_async_copy(vir_hbm, vir_ref, pair_sem.at[1])
    ]
    energy_copies = [
        pltpu.make_async_copy(occ_energy_hbm, occ_energy_ref, energy_sem.at[0]),
        pltpu.make_async_copy(vir_energy_hbm, vir_energy_ref, energy_sem.at[1]),
    ]
    barrier = pltpu.get_barrier_semaphore()
    for index in range(1, 8):
        pl.semaphore_signal(barrier, inc=1, device_id=peer(index), device_id_type=MESH)
    for copy in pair_copies:
        copy.start()
    for b in range(2):
        amp_copy(b).start()
        lad_copy(0, b, True).start()
    for copy in pair_copies:
        copy.wait()

    def keep_of(b, column0, width):
        row = lax.broadcasted_iota(jnp.int32, (rows, width), 0)
        column = me * cols + column0 + lax.broadcasted_iota(jnp.int32, (rows, width), 1)
        return (row < occ_ref[first + b]) & (column < vir_ref[first + b])

    def mask(b):
        amp_copy(b).wait()
        shape = (16, LANES)
        lane = me * cols + lax.broadcasted_iota(jnp.int32, shape, 1)
        masks = [
            jnp.where(lane + g * LANES < vir_ref[first + b], 1.0, 0.0).astype(jnp.bfloat16) for g in range(cols // LANES)
        ]

        def one(index, carry):
            row0 = pl.multiple_of(index * 16, 16)
            row = row0 + lax.broadcasted_iota(jnp.int32, shape, 0)
            live = jnp.where(row < occ_ref[first + b], 1.0, 0.0).astype(jnp.bfloat16)
            for g in range(cols // LANES):
                lanes = slice(g * LANES, (g + 1) * LANES)
                amp[b, pl.ds(row0, 16), lanes] = amp[b, pl.ds(row0, 16), lanes] * masks[g] * live
            return carry

        lax.fori_loop(0, rows // 16, one, 0)

    for n in range(2, lad_slots):
        lad_copy(n // 4, n % 4, True).start()
    hole_copy.start()
    for copy in energy_copies:
        copy.start()
    twice(mask)
    pl.semaphore_wait(barrier, 7)

    def part(step, k, is_small):
        lad_copy(step, k, is_small).wait()
        width = small if is_small else big
        return jnp.dot(amp[k % 2], lad[(4 * step + k) % lad_slots, :, 0:width], preferred_element_type=jnp.float32)

    def refill(step, k, is_small):
        ahead = 4 * step + k + lad_slots
        later, k_later = step + (k + lad_slots) // 4, (k + lad_slots) % 4
        if is_small:

            @pl.when(later < first_big)
            def _():
                lad_copy(later, k_later, True).start()

            @pl.when(later >= first_big)
            def _():
                lad_copy(later, k_later, False).start()
        else:

            @pl.when(later < steps)
            def _():
                lad_copy(later, k_later, False).start()

    def produce(step, is_small):
        target, spare = (parts_small, 2 * first_big) if is_small else (parts, 4)

        def one(k, carry):
            b, theirs = k % 2, k < 2
            if not is_small:

                @pl.when(theirs & (step >= first_big + 2))
                def _():
                    core_copy(step - 2, b, False).wait_send()

            given = step * 2 + b if is_small else (step % 2) * 2 + b
            target[jnp.where(theirs, given, spare + b)] = part(step, k, is_small)

            @pl.when(theirs)
            def _():
                core_copy(step, b, is_small).start()

            refill(step, k, is_small)
            return carry

        lax.fori_loop(0, 4, one, 0)

    def lanes_of(g):
        return slice(g * LANES, (g + 1) * LANES)

    def both_cores(step, b, g, is_small):
        source, at = (core_in_small, step * 2 + b) if is_small else (core_in, (step - first_big) * 2 + b)
        own, slot = (parts_small, 2 * first_big + b) if is_small else (parts, 4 + b)
        return own[slot, :, lanes_of(g)] + source[at, :, lanes_of(g)]

    def scales_of(kind, at):
        top = widths[kind] // LANES * rows
        codes = ins[kind][at, top : top + HALF_TILE, :].astype(jnp.int32).astype(jnp.float32)
        return jnp.exp2(codes * (1.0 / GRID_STEPS)) * (1.0 / TOP)

    def decoded(kind, at, scales, g):
        return ins[kind][at, g * rows : (g + 1) * rows, :].astype(jnp.int32).astype(jnp.float32) * scales[g : g + 1, :]

    def send(kind, at, values, target):
        out = outs[kind]
        codes = jnp.zeros((HALF_TILE, LANES), jnp.float32)
        which = lax.broadcasted_iota(jnp.int32, (HALF_TILE, LANES), 0)
        groups = widths[kind] // LANES
        for g in range(groups):
            value = values(g)
            largest = jnp.max(jnp.abs(value), axis=0, keepdims=True)
            code = jnp.ceil(jnp.log2(jnp.maximum(largest, 1e-30)) * GRID_STEPS) + 1.0
            scaled = value * (jnp.exp2(code * (-1.0 / GRID_STEPS)) * TOP)
            out[at, g * rows : (g + 1) * rows, :] = jnp.round(scaled).astype(jnp.int32).astype(jnp.int16)
            codes = jnp.where(which == g, jnp.broadcast_to(code, (HALF_TILE, LANES)), codes)
        out[at, groups * rows : groups * rows + HALF_TILE, :] = codes.astype(jnp.int32).astype(jnp.int16)
        link_copy(kind, at, target).start()

    def send_small(step, carry):
        produce(step, True)

        def one(b):
            core_copy(step, b, True).wait_recv()
            send(SMALL, step * 2 + b, lambda g: both_cores(step, b, g, True), near_side(b))

        twice(one)
        return carry

    def send_whole(step, carry):
        produce(step, False)

        def one(b):
            core_copy(step, b, False).wait_recv()
            at = (step - first_big) * 2 + b
            send(WHOLE, at, lambda g: both_cores(step, b, g, False), near_side(b))

        twice(one)
        return carry

    def send_joined(half, carry):
        step = first_big + 2 + half
        produce(step, False)

        def one(b):
            core_copy(step, b, False).wait_recv()
            arrived = []
            for piece in range(3):
                at = 2 * (half * 3 + piece) + b
                link_copy(SMALL, at, near_side(b)).wait_recv()
                scales = scales_of(SMALL, at)
                arrived += [(SMALL, at, scales, g) for g in range(small // LANES)]

            def value(g):
                return both_cores(step, b, g, False) + decoded(*arrived[g])

            head = widths[HEAD] // LANES
            send(HEAD, half * 2 + b, value, far_side(b))
            send(LAST, half * 2 + b, lambda g: value(head + g), far_side(b))

        twice(one)
        return carry

    def gap_of(b, column):
        both = vir_energy_ref[:, pl.ds(column, LANES)]
        return jnp.where(b == 0, both[0:1], both[1:2]) - occ_wide[b]

    def keep_base(step, carry):
        produce(step, False)
        start = (step - (steps - 2)) * big

        def one(b):
            from_hole = jnp.dot(
                hole[b], amp[b, :, pl.ds(pl.multiple_of(start, LANES), big)], preferred_element_type=jnp.float32
            )
            core_copy(step, b, False).wait_recv()
            for g in range(big // LANES):
                at = pl.multiple_of(start + g * LANES, LANES)
                wide = amp[b, :, pl.ds(at, LANES)].astype(jnp.float32)
                total = both_cores(step, b, g, False) + from_hole[:, lanes_of(g)] + gap_of(b, at) * wide
                core_in[(step - first_big) * 2 + b, :, lanes_of(g)] = total

        twice(one)
        return carry

    def settle(half, carry):
        def one(b):
            at = half * 2 + b
            link_copy(WHOLE, at, near_side(b)).wait_recv()
            scales = scales_of(WHOLE, at)
            base = (steps - 2 - first_big + half) * 2 + b
            for g in range(big // LANES):
                core_in[base, :, lanes_of(g)] = core_in[base, :, lanes_of(g)] + decoded(WHOLE, at, scales, g)

        twice(one)
        return carry

    def residual_of(kind, half, skip):
        def one(b):
            link_copy(kind, half * 2 + b, far_side(b)).wait_recv()
            scales = scales_of(kind, half * 2 + b)
            base = (steps - 2 - first_big + half) * 2 + b
            for g in range(widths[kind] // LANES):
                at = pl.multiple_of(half * big + (skip + g) * LANES, LANES)
                total = core_in[base, :, lanes_of(skip + g)] + decoded(kind, half * 2 + b, scales, g)
                residual = jnp.where(keep_of(b, at, LANES), total, 0.0)
                core_in[base, :, lanes_of(skip + g)] = residual
                squares[b] = squares[b] + jnp.sum((residual * residual).reshape(rows // 8, 8, LANES), axis=0)

        twice(one)

    def update_of(kind, half, skip):
        def one(b):
            base = (steps - 2 - first_big + half) * 2 + b
            for g in range(widths[kind] // LANES):
                at = pl.multiple_of(half * big + (skip + g) * LANES, LANES)
                wide = amp[b, :, pl.ds(at, LANES)].astype(jnp.float32)
                new = wide - core_in[base, :, lanes_of(skip + g)] / (gap_of(b, at) + LEVEL_SHIFT)
                out_ref[b, :, pl.ds(at, LANES)] = new.astype(jnp.bfloat16)

        twice(one)

    lax.fori_loop(0, first_big, send_small, 0)
    lax.fori_loop(first_big, first_big + 2, send_whole, 0)
    lax.fori_loop(0, 2, send_joined, 0)
    hole_copy.wait()
    for copy in energy_copies:
        copy.wait()
    for b in range(2):
        occ_wide[b] = jnp.broadcast_to(occ_energy_ref[b : b + 1, :], (LANES, rows)).T
    lax.fori_loop(steps - 2, steps, keep_base, 0)
    lax.fori_loop(0, 2, settle, 0)
    head = widths[HEAD] // LANES
    for b in range(2):
        squares[b] = jnp.zeros((8, LANES), jnp.float32)
        counts_ref[b] = jnp.full((8, LANES), (occ_ref[first + b] * vir_ref[first + b]).astype(jnp.float32), jnp.float32)

    def finish(half, carry):
        residual_of(HEAD, half, 0)
        update_of(HEAD, half, 0)
        residual_of(LAST, half, head)

        @pl.when(half == 0)
        def _():
            update_of(LAST, half, head)

        return carry

    lax.fori_loop(0, 2, finish, 0)
    for b in range(2):
        flat[b : b + 1, :] = jnp.sum(squares[b], axis=0, keepdims=True)
    squares_in[me] = flat[...]
    for index in (5, 7, 3, 4, 6, 1, 2):
        square_copy(index, me, peer(index)).start()
    update_of(LAST, 1, head)
    for kind in range(4):
        for at in range(outs[kind].shape[0]):
            link_copy(kind, at, near_side(0)).wait_send()
    for b in range(2):
        for step in range(first_big):
            core_copy(step, b, True).wait_send()
        for step in (steps - 2, steps - 1):
            core_copy(step, b, False).wait_send()
    for index in range(1, 8):
        square_copy(index, me, peer(index)).wait_send()
    for index in range(1, 8):
        square_copy(index, square_source(index), peer(index)).wait_recv()


def emit_kernel(updated, squares, counts, out_hbm, norm_hbm, norm_ref, norm_sem, sem):
    band = updated.shape[1] // BANDS
    copies = [
        pltpu.make_async_copy(updated.at[b, pl.ds(i * band, band)], out_hbm.at[b, pl.ds(i * band, band)], sem.at[b * BANDS + i])
        for b in range(2)
        for i in range(BANDS)
    ]
    for copy in copies:
        copy.start()
    for b in range(2):
        total = squares[0, b : b + 1, :]
        for index in range(1, squares.shape[0]):
            total = total + squares[index, b : b + 1, :]
        total = jnp.full((8, LANES), jnp.sum(total), jnp.float32)
        norm_ref[b] = jnp.sqrt(total / counts[b] + EPSILON)[0, 0]
    copies.append(pltpu.make_async_copy(norm_ref, norm_hbm, norm_sem))
    copies[-1].start()
    for copy in copies:
        copy.wait()


def group_body(amplitudes, ladder_ints, hole_ints, occ_energy, vir_energy, occ_pairs, vir_pairs):
    blocks, rows, cols = amplitudes.shape
    big = cols // 2
    small = big // 3
    units = ((12, small), (4, big), (4, big - LANES), (4, LANES))
    coded = [pltpu.VMEM((count, width // LANES * rows + HALF_TILE, LANES), jnp.int16) for count, width in units]
    anywhere = pl.BlockSpec(memory_space=pl.ANY)
    vmem = pl.BlockSpec(memory_space=pltpu.VMEM)
    smem = pl.BlockSpec(memory_space=pltpu.SMEM)
    dma = pltpu.SemaphoreType.DMA
    sems = [dma((count,)) for count, _ in units]
    outs = pl.pallas_call(
        functools.partial(group_kernel, (rows, cols)),
        in_specs=[anywhere] * 7,
        out_specs=[vmem] * 3,
        out_shape=[
            pltpu.VMEM((blocks, rows, cols), jnp.bfloat16),
            pltpu.VMEM((8, blocks, LANES), jnp.float32),
            pltpu.VMEM((blocks, 8, LANES), jnp.float32),
        ],
        scratch_shapes=[
            pltpu.VMEM((2, rows, cols), jnp.bfloat16),
            pltpu.VMEM((2, rows, rows), jnp.bfloat16),
            pltpu.VMEM((2, rows, LANES), jnp.float32),
            pltpu.VMEM((6, cols, big), jnp.bfloat16),
            pltpu.VMEM((14, rows, small), jnp.float32),
            pltpu.VMEM((6, rows, big), jnp.float32),
            pltpu.VMEM((12, rows, small), jnp.float32),
            pltpu.VMEM((12, rows, big), jnp.float32),
            pltpu.VMEM((2, 8, LANES), jnp.float32),
            pltpu.VMEM((2, LANES), jnp.float32),
            pltpu.SMEM(occ_pairs.shape, jnp.int32),
            pltpu.SMEM(vir_pairs.shape, jnp.int32),
            pltpu.VMEM(occ_energy.shape, jnp.float32),
            pltpu.VMEM(vir_energy.shape, jnp.float32),
            dma((2,)), dma((2,)),
            dma((2,)), dma(()), dma((6,)), dma((12,)), dma((4,)), dma((12,)), dma((12,)), dma((7,)), dma((8,)),
            *coded, *coded, *sems, *sems,
        ],
        compiler_params=pltpu.CompilerParams(
            collective_id=0, has_side_effects=True, vmem_limit_bytes=VMEM_BYTES
        ),
        name="ladder_group",
    )(occ_pairs, vir_pairs, amplitudes, ladder_ints, hole_ints, occ_energy, vir_energy)
    return pl.pallas_call(
        emit_kernel,
        in_specs=[vmem] * 3,
        out_specs=[anywhere] * 2,
        out_shape=[
            jax.ShapeDtypeStruct((blocks, rows, cols), jnp.bfloat16),
            jax.ShapeDtypeStruct((blocks,), jnp.float32),
        ],
        scratch_shapes=[pltpu.SMEM((blocks,), jnp.float32), dma(()), dma((2 * BANDS,))],
        compiler_params=pltpu.CompilerParams(vmem_limit_bytes=2**20),
        name="emit",
    )(*outs)


def solution(mesh):
    in_specs = (
        P("irrep", None, SLOTS),
        P("irrep", SLOTS, None),
        P("irrep", None, None),
        P("irrep", None),
        P("irrep", SLOTS),
        P(),
        P(),
    )
    out_specs = (P("irrep", None, SLOTS), P("irrep"))

    def chosen(amplitudes, *rest):
        return (group_body if fits_group(mesh, amplitudes.shape[2]) else body)(amplitudes, *rest)

    return jax.shard_map(chosen, mesh=mesh, in_specs=in_specs, out_specs=out_specs, check_vma=False)
```
